32 devices in a mesh: seq: 8 (over z, x), batch: 4 (over y, core).
Axes of the slice: x: 2, y: 2, z: 4, core: 2. Of those that a mesh axis runs over, the one named last changes fastest.
Arguments:
- inputs: bfloat16 [4, 2048, 6144], P('batch', 'seq'), may hold values from -6 to 6
- out_grad: bfloat16 [4, 2048, 6144], P('batch', 'seq'), may hold values from -6 to 6
- step_size: float32 [4, 96, 2048], P('batch', None, 'seq'), may hold values from 0.5 to 2
- log_decay: float32 [4, 96, 2048], P('batch', None, 'seq'), may hold values from -1 to 0
- b_matrix: bfloat16 [4, 16, 2048], P('batch', None, 'seq'), may hold values from -1.5 to 1.5
- c_matrix: bfloat16 [4, 16, 2048], P('batch', None, 'seq'), may hold values from -0.125 to 0.125
- skip_gain: float32 [96], replicated, may hold values from 0.5 to 1.5
- lengths: int32 [4], P('batch'), may hold values from 256 to 2048
Outputs:
- grad_x: bfloat16 [4, 2048, 6144], P('batch', 'seq')
- grad_b: float32 [4, 16, 2048], P('batch', None, 'seq')
- grad_c: float32 [4, 16, 2048], P('batch', None, 'seq')
The draws below stay inside these ranges and needn't reach their ends.
All inputs are finite; a program needn't handle non-finite values.
Results may differ from the reference program's by a relative error of at most 0.0047.
Values may be sent and summed in bfloat16 or wider, within the bound.
No kernel may reach another device: no remote copies, remote signals or barrier semaphores. Data moves between devices by JAX's collectives and lax.ppermute only.
A program may use at most 128 MiB of HBM per device.

```python
import math
import jax
import jax.numpy as jnp
from jax import lax

HEADS = 96
HEAD_DIM = 64
STATE = 16
SPAN = 256
TOK_DEV = 256
SEQ_LEN = 2048
SEQS = 4


def draw_log_decay(key, part):
    keys = jax.random.split(jax.random.fold_in(key, 11), 7)
    steady_share = 0.5
    shards = SEQ_LEN // TOK_DEV
    steady = jax.random.uniform(keys[0], (SEQS, HEADS), jnp.float32) < steady_share
    slow_rate = jnp.exp(jax.random.uniform(keys[1], (SEQS, HEADS), jnp.float32, jnp.log(0.1), jnp.log(0.5))) / SEQ_LEN
    block_factor = jnp.exp(jax.random.uniform(keys[3], (SEQS, HEADS, shards), jnp.float32, jnp.log(0.5), jnp.log(2.0)))
    still = jax.random.uniform(keys[6], (SEQS, HEADS, shards), jnp.float32) < 0.5
    varied_rate = jnp.exp(jax.random.uniform(keys[2], (SEQS, HEADS, shards), jnp.float32, jnp.log(0.3 / TOK_DEV), jnp.log(0.04)))
    drawn_rate = slow_rate[:, :, None] * block_factor
    keeps_state = jnp.logical_or(steady[:, :, None], still)
    shard_rate = jnp.where(keeps_state, drawn_rate, varied_rate)
    shard_rate = jnp.repeat(shard_rate, TOK_DEV, axis=2)
    roughness = jax.random.uniform(keys[4], (SEQS, HEADS, SEQ_LEN), jnp.float32, 0.5, 1.5)
    recurrence_moves = -shard_rate * roughness
    flagged_places = jax.random.randint(jax.random.fold_in(keys[5], 3), (SEQS, 2), 0, SEQ_LEN)
    element_locations = lax.iota(jnp.int32, SEQ_LEN)
    spell_tallies = jnp.any(element_locations[None, None, :] == flagged_places[:, :, None], axis=1)
    excluded_lines = jax.random.uniform(jax.random.fold_in(keys[5], 7), (SEQS, 1, SEQ_LEN), jnp.float32, 0.22, 0.69)
    return recurrence_moves - jnp.where(spell_tallies[:, None, :], excluded_lines, 0.0)


def touch_ends(result, rng, least, largest):
    extent = result.shape
    spot = [jax.random.randint(jax.random.fold_in(rng, axis), (), 0, extent[axis]) for axis in range(len(extent))]
    result = result.at[tuple(spot)].set(least)
    longest = extent.index(max(extent))
    spot[longest] = (spot[longest] + 1) % extent[longest]
    return result.at[tuple(spot)].set(largest)


def block_levels(key, dims, cuts, least, high):
    def one(position, shards_of):
        steps = jax.random.uniform(jax.random.fold_in(jax.random.fold_in(key, 6), position), (shards_of,), jnp.float32, least / len(cuts), high / len(cuts))
        return jnp.repeat(jnp.exp(steps), dims[position] // shards_of).reshape((-1,) + (1,) * (len(dims) - position - 1))

    level = one(*cuts[0])
    for cut in cuts[1:]:
        level = level * one(*cut)
    return level


def noise(key, shape, spread, most, cuts=(), kind=jnp.bfloat16):
    result = jax.random.normal(key, shape, jnp.float32) * spread
    if len(cuts) > 0:
        result = block_levels(key, shape, cuts, -0.22, 0.18) * result
    return jnp.clip(result, min=-most, max=most).astype(kind)


def setup_inputs(seed: int = 0) -> dict:
    splits = jax.random.split(jax.random.key(seed), 9)
    return {
        "inputs": noise(splits[0], (SEQS, SEQ_LEN, HEADS * HEAD_DIM), 1.0, 6.0, ((0, 4), (1, 8))),
        "out_grad": noise(splits[1], (SEQS, SEQ_LEN, HEADS * HEAD_DIM), 1.0, 6.0, ((0, 4), (1, 8))),
        "step_size": jnp.clip(jnp.exp(math.log(2.0) - 1.3862944 * jax.random.uniform(splits[2], (SEQS, HEADS, SEQ_LEN), jnp.float32) ** block_levels(splits[2], (SEQS, HEADS, SEQ_LEN), ((0, 4), (2, 8)), -0.2, 0.2)), 0.5, 2.0),
        "log_decay": draw_log_decay(jax.random.fold_in(splits[8], 71), 0),
        "b_matrix": noise(splits[4], (SEQS, STATE, SEQ_LEN), STATE ** -0.5, 1.5, ((0, 4), (2, 8))),
        "c_matrix": noise(splits[5], (SEQS, STATE, SEQ_LEN), SEQ_LEN ** -0.5, 0.125, ((0, 4), (2, 8))),
        "skip_gain": jnp.clip(jax.random.uniform(splits[6], (HEADS,), jnp.float32, 0.5, 1.5), 0.5, 1.5),
        "lengths": touch_ends(jax.random.randint(splits[7], (SEQS,), TOK_DEV, SEQ_LEN + 1), jax.random.fold_in(splits[7], 1), TOK_DEV, SEQ_LEN).astype(jnp.int32),
    }


HIGHEST = lax.Precision.HIGHEST


def rounded(values):
    return lax.optimization_barrier(values.astype(jnp.bfloat16)).astype(jnp.float32)


def block_summary(inputs, masked, step_size, cumulative, b_matrix, c_matrix):
    row_count, columns = inputs.shape
    head_count = step_size.shape[0]
    x_heads = inputs.reshape(row_count, head_count, columns // head_count).astype(jnp.float32)
    dy_heads = masked.reshape(row_count, head_count, columns // head_count).astype(jnp.float32)
    to_end = jnp.exp(cumulative[:, -1:] - cumulative)
    into_state = rounded(b_matrix.astype(jnp.float32)[None] * (to_end * step_size)[:, None, :])
    into_grad = rounded(c_matrix.astype(jnp.float32)[None] * jnp.exp(cumulative)[:, None, :])
    state_part = jnp.einsum("hnu,uhp->hnp", into_state, x_heads, precision=HIGHEST)
    grad_part = jnp.einsum("hnu,uhp->hnp", into_grad, dy_heads, precision=HIGHEST)
    return jnp.exp(cumulative[:, -1]), state_part, grad_part


def block_grads(inputs, masked, step_size, cumulative, b_matrix, c_matrix, incoming_state, grad_in, skip_gain, scale_b, scale_c):
    row_count, columns = inputs.shape
    head_count = step_size.shape[0]
    head_dim = columns // head_count
    x_heads = inputs.reshape(row_count, head_count, head_dim).astype(jnp.float32)
    dy_heads = masked.reshape(row_count, head_count, head_dim).astype(jnp.float32)
    to_end = jnp.exp(cumulative[:, -1:] - cumulative)
    from_start = jnp.exp(cumulative)
    row_ids = lax.broadcasted_iota(jnp.int32, (row_count, row_count), 0)
    col_ids = lax.broadcasted_iota(jnp.int32, (row_count, row_count), 1)
    differences = cumulative[:, :, None] - cumulative[:, None, :]
    forward_decay = jnp.exp(jnp.where((row_ids >= col_ids)[None], differences, -jnp.inf))
    c_dot_b = jnp.dot(c_matrix.T, b_matrix, preferred_element_type=jnp.float32)
    kernel = rounded(forward_decay * c_dot_b[None])
    grad16 = rounded(grad_in)
    state16 = rounded(incoming_state)
    b_wide = b_matrix.astype(jnp.float32)
    c_wide = c_matrix.astype(jnp.float32)
    within = jnp.einsum("hut,uhp->thp", kernel, dy_heads, precision=HIGHEST)
    across = jnp.einsum("nt,hnp->thp", b_wide, grad16, precision=HIGHEST) * to_end.T[:, :, None]
    grad_x = step_size.T[:, :, None] * (within + across) + skip_gain[None, :, None] * dy_heads
    scores = jnp.einsum("thp,uhp->htu", x_heads, dy_heads, precision=HIGHEST)
    mixing = jnp.sum(step_size[:, :, None] * jnp.swapaxes(forward_decay, 1, 2) * scores, axis=0)
    cross_b = jnp.einsum("htn,ht->nt", jnp.einsum("thp,hnp->htn", x_heads, grad16, precision=HIGHEST), step_size * to_end, precision=HIGHEST)
    across_c_terms = jnp.einsum("htn,ht->nt", jnp.einsum("thp,hnp->htn", dy_heads, state16, precision=HIGHEST), from_start, precision=HIGHEST)
    grad_b = (jnp.dot(c_wide, mixing.T, precision=HIGHEST) + cross_b) * scale_b
    grad_c = (jnp.dot(b_wide, mixing, precision=HIGHEST) + across_c_terms) * scale_c
    return grad_x.reshape(row_count, columns).astype(jnp.bfloat16), grad_b, grad_c


def sequence_grads(inputs, out_grad, step_size, log_decay, b_matrix, c_matrix, length, skip_gain):
    seq_rows, columns = inputs.shape
    head_count = step_size.shape[0]
    state_size = b_matrix.shape[0]
    blocks = seq_rows // SPAN
    interior = lax.iota(jnp.int32, seq_rows) < length
    masked = jnp.where(interior[:, None], out_grad, jnp.zeros_like(out_grad))
    x_blocks = inputs.reshape(blocks, SPAN, columns)
    dy_blocks = masked.reshape(blocks, SPAN, columns)
    dt_blocks = step_size.reshape(head_count, blocks, SPAN).transpose(1, 0, 2)
    cumulative = jnp.cumsum(log_decay.reshape(head_count, blocks, SPAN), axis=2).transpose(1, 0, 2)
    b_blocks = b_matrix.reshape(state_size, blocks, SPAN).transpose(1, 0, 2)
    c_blocks = c_matrix.reshape(state_size, blocks, SPAN).transpose(1, 0, 2)
    decays, state_parts, grad_parts = lax.map(lambda element: block_summary(*element), (x_blocks, dy_blocks, dt_blocks, cumulative, b_blocks, c_blocks))

    def pass_on(running, element):
        factor, portion = element
        return factor[:, None, None] * running + portion, running

    initial = jnp.zeros((head_count, state_size, columns // head_count), jnp.float32)
    _, state_ins = lax.scan(pass_on, initial, (decays, state_parts))
    _, grad_ins = lax.scan(pass_on, initial, (decays, grad_parts), reverse=True)
    scale_b = 1.0 / float(columns) ** 0.5
    scale_c = (float(state_size) / float(columns * seq_rows)) ** 0.5
    grad_x, grad_b, grad_c = lax.map(lambda element: block_grads(*element, skip_gain, scale_b, scale_c), (x_blocks, dy_blocks, dt_blocks, cumulative, b_blocks, c_blocks, state_ins, grad_ins))
    grad_b = grad_b.transpose(1, 0, 2).reshape(state_size, seq_rows)
    grad_c = grad_c.transpose(1, 0, 2).reshape(state_size, seq_rows)
    return grad_x.reshape(seq_rows, columns), grad_b, grad_c


def reference(inputs, out_grad, step_size, log_decay, b_matrix, c_matrix, skip_gain, lengths):
    grad_x, grad_b, grad_c = lax.map(lambda element: sequence_grads(*element, skip_gain), (inputs, out_grad, step_size, log_decay, b_matrix, c_matrix, lengths))
    return grad_x, grad_b, grad_c
```

```python
import functools
import math

import jax
import jax.numpy as jnp
from jax import lax
from jax.experimental import pallas as pl
from jax.experimental.pallas import tpu as pltpu
from jax.sharding import PartitionSpec as P

SPAN = 256
LANES = 128
LOG2E = math.log2(math.e)
F32 = jnp.float32
BF16 = jnp.bfloat16
VM = pltpu.VMEM
ANY = pl.ANY


def place():
    idx = lax.axis_index("seq")
    count = lax.axis_size("seq")
    return idx, lax.rem(idx, 2), idx < count // 2


def valid_rows(len_ref, tokens):
    return len_ref[0] - lax.axis_index("seq") * tokens


def lane_low(shape, head_dim):
    return lax.broadcasted_iota(jnp.int32, shape, 1) < head_dim


def running_sum(values):
    rows, span = values.shape
    high = values.astype(BF16)
    rest = values - high.astype(F32)
    middle = rest.astype(BF16)
    low = (rest - middle.astype(F32)).astype(BF16)
    upper = lax.broadcasted_iota(jnp.int32, (span, span), 0) <= lax.broadcasted_iota(
        jnp.int32, (span, span), 1
    )
    pieces = jnp.concatenate([high, middle, low], axis=0)
    sums = jnp.dot(pieces, upper.astype(BF16), preferred_element_type=F32)
    return sums[:rows] + sums[rows : 2 * rows] + sums[2 * rows :]


def weights(ld, dt, valid):
    cum = running_sum(ld)
    end = cum[:, -1:]
    inside = lax.broadcasted_iota(jnp.int32, cum.shape, 1) < valid
    into_state = dt * jnp.exp(end - cum)
    into_grad = jnp.where(inside, jnp.exp(cum), 0.0)
    return end, into_state, into_grad


def summary_kernel(tasks, head_dim, len_ref, ld_ref, dt_ref, b_ref, c_ref, x_ref, dy_ref, *refs):
    outs = refs[: len(tasks)]
    decay_ref, buf_ref, w_ref, spread_ref, sems = refs[len(tasks) :]
    idx, mine, lower = place()
    heads, span = ld_ref.shape
    half_heads = heads // 2
    width = half_heads * head_dim
    chunks = sems.shape[1]
    chunk = width // chunks
    kinds = [lower if first else jnp.logical_not(lower) for first, own in tasks]
    halves = [mine if own else 1 - mine for first, own in tasks]

    def copy(t, i, src):
        start = pl.multiple_of(halves[t] * width + i * chunk, LANES)
        return pltpu.make_async_copy(
            src.at[:, pl.ds(start, chunk)],
            buf_ref.at[t, :, pl.ds(i * chunk, chunk)],
            sems.at[t, i],
        )

    for t in range(len(tasks)):
        for i in range(chunks):

            @pl.when(kinds[t])
            def _():
                copy(t, i, x_ref).start()

            @pl.when(jnp.logical_not(kinds[t]))
            def _():
                copy(t, i, dy_ref).start()

    valid = valid_rows(len_ref, span)
    low = lane_low((STATE_ROWS(b_ref), LANES), head_dim)
    done = {}
    for own in sorted({own for first, own in tasks}):
        half = mine if own else 1 - mine
        rows = pl.ds(pl.multiple_of(half * half_heads, 8), half_heads)
        done[own] = weights(ld_ref[rows, :], dt_ref[rows, :], valid)
    decay_half = tasks[0][1]
    spread_ref[...] = jnp.broadcast_to(jnp.exp(done[decay_half][0]), (half_heads, LANES))
    pairs = half_heads // 2
    even = spread_ref[pl.ds(0, pairs, stride=2), :]
    odd = spread_ref[pl.ds(1, pairs, stride=2), :]
    spread = jnp.where(lane_low((pairs, LANES), head_dim), even, odd)
    if decay_half:
        decay_ref[...] = spread
    else:
        high = spread.astype(BF16).astype(F32)
        both = jnp.concatenate([high, spread - high], axis=0).astype(BF16)
        decay_ref[...] = both.reshape(decay_ref.shape)
    for t, (first, own) in enumerate(tasks):
        end, into_state, into_grad = done[own]
        w_ref[t] = jnp.where(kinds[t], into_state, into_grad)
        mat = jnp.where(kinds[t], b_ref[...].astype(F32), c_ref[...].astype(F32))
        states = mat.shape[0]
        per = 2 * LANES // head_dim
        for i in range(chunks):
            copy(t, i, x_ref).wait()
            for g in range(i * chunk // (2 * LANES), (i + 1) * chunk // (2 * LANES)):
                lhs = jnp.concatenate(
                    [
                        (mat * w_ref[t, pl.ds(per * g + j, 1), :]).astype(BF16)
                        for j in range(per)
                    ],
                    axis=0,
                )
                rhs = buf_ref[t, :, pl.ds(2 * LANES * g, 2 * LANES)]
                res = jnp.dot(lhs, rhs, preferred_element_type=F32)
                for q in range(2):
                    top = res[2 * q * states : (2 * q + 1) * states, q * LANES : (q + 1) * LANES]
                    bottom = res[
                        (2 * q + 1) * states : (2 * q + 2) * states, q * LANES : (q + 1) * LANES
                    ]
                    outs[t][2 * g + q] = jnp.where(low, top, bottom).astype(outs[t].dtype)


def STATE_ROWS(ref):
    return ref.shape[0]


def summary(tasks, types, length, ld, dt, b, c, x, dy):
    heads, span = ld.shape
    columns = x.shape[1]
    head_dim = columns // heads
    states = b.shape[0]
    tiles = columns // 2 // LANES
    pairs = heads // 4
    if tasks[0][1]:
        decay = jax.ShapeDtypeStruct((pairs, LANES), F32)
    else:
        decay = jax.ShapeDtypeStruct((2 * pairs // states, states, LANES), BF16)
    whole = lambda: pl.BlockSpec(memory_space=VM)
    count = len(tasks)
    return pl.pallas_call(
        functools.partial(summary_kernel, tasks, head_dim),
        out_shape=[jax.ShapeDtypeStruct((tiles, states, LANES), t) for t in types] + [decay],
        in_specs=[pl.BlockSpec(memory_space=pltpu.SMEM)]
        + [whole() for _ in range(4)]
        + [pl.BlockSpec(memory_space=ANY)] * 2,
        out_specs=[whole() for _ in range(count + 1)],
        scratch_shapes=[
            pltpu.VMEM((count, span, columns // 2), BF16),
            pltpu.VMEM((count, heads // 2, span), F32),
            pltpu.VMEM((heads // 2, LANES), F32),
            pltpu.SemaphoreType.DMA((count, 4)),
        ],
        compiler_params=pltpu.CompilerParams(vmem_limit_bytes=(4 + 4 * count) << 20),
        name="summary",
    )(length, ld, dt, b, c, x, dy)


def pair_flags(second):
    idx, mine, lower = place()
    ahead = jnp.where(lower, mine == 0, mine == 1)
    return jnp.logical_not(ahead) if second else ahead


def partner_rows(decay_ref):
    count = decay_ref.shape[0] * decay_ref.shape[1]
    both = decay_ref[...].reshape(count, LANES).astype(F32)
    return both[: count // 2] + both[count // 2 :]


def chain_kernel(second, carries, finish, msg, *refs):
    refs = list(refs)
    decay_ref, mine_ref, x_ref, y_ref = refs[:4]
    carry_refs = refs[4 : 4 + carries]
    rest = refs[4 + carries :]
    ahead = pair_flags(second)
    tiles = x_ref.shape[0]
    dp_ref = rest[-1]
    dp_ref[...] = partner_rows(decay_ref)
    for j in range(tiles):
        dp = dp_ref[pl.ds(j, 1), :]
        d = mine_ref[pl.ds(j, 1), :]
        x = x_ref[j]
        y = y_ref[j].astype(F32)
        carry = None
        for ref in carry_refs:
            carry = ref[j].astype(F32) if carry is None else carry + ref[j].astype(F32)
        at = 0
        if msg:
            total = jnp.where(ahead, dp, d) * jnp.where(ahead, x, y) + jnp.where(ahead, y, x)
            if carry is not None:
                total = total + d * dp * carry
            rest[at][j] = total.astype(BF16)
            at += 1
        if finish:
            if carry is None:
                carry = jnp.zeros_like(x)
            passed = jnp.where(ahead, d, dp) * carry + jnp.where(ahead, x, y)
            own = jnp.where(ahead, carry, passed)
            send = jnp.where(ahead, passed, carry)
            rest[at][j] = own.astype(BF16)
            rest[at + 1][j] = send.astype(BF16)


def chain(second, decay, mine, x, y, carries, msg, finish):
    shape = jax.ShapeDtypeStruct(x.shape, BF16)
    outs = int(msg) + 2 * int(finish)
    whole = lambda: pl.BlockSpec(memory_space=VM)
    return pl.pallas_call(
        functools.partial(chain_kernel, second, len(carries), finish, msg),
        out_shape=[shape] * outs,
        in_specs=[whole() for _ in range(4 + len(carries))],
        out_specs=[whole() for _ in range(outs)],
        scratch_shapes=[pltpu.VMEM(mine.shape, F32)],
        compiler_params=pltpu.CompilerParams(vmem_limit_bytes=4 << 20),
        name="chain",
    )(decay, mine, x, y, *carries)


def intra_kernel(head0, per_step, head_dim, first, len_ref, skip_ref, *refs):
    if first:
        ld_ref, dt_ref, b_ref, c_ref, x_ref, dy_ref = refs[:6]
        rest = refs[6:]
    else:
        ld_ref, dt_ref, b_ref, c_ref, x_ref, dy_ref, mix_in, part_in = refs[:8]
        rest = refs[8:]
    part_ref, mix_ref, cb_ref, row_ref, col_ref = rest
    span = x_ref.shape[0]
    half = span // 2
    valid = valid_rows(len_ref, span)
    step = pl.program_id(0)
    call_heads = row_ref.shape[0]

    @pl.when(step == 0)
    def _():
        if first:
            mix_ref[...] = jnp.zeros_like(mix_ref)
        else:
            mix_ref[...] = mix_in[...]
        t = lax.broadcasted_iota(jnp.int32, (span, span), 0)
        u = lax.broadcasted_iota(jnp.int32, (span, span), 1)
        dots = lax.dot_general(
            b_ref[...], c_ref[...], (((0,), (0,)), ((), ())), preferred_element_type=F32
        )
        cb_ref[...] = jnp.where(jnp.logical_and(u >= t, u < valid), dots, 0.0)
        cum = running_sum(ld_ref[pl.ds(head0, call_heads), :]) * LOG2E
        row_ref[...] = cum
        shifted = cum - jnp.log(dt_ref[pl.ds(head0, call_heads), :]) * LOG2E
        col_ref[...] = shifted.T

    lane = lax.broadcasted_iota(jnp.int32, (1, LANES), 1)
    keep0 = (lane < head_dim).astype(BF16)
    keep1 = (lane >= head_dim).astype(BF16)
    low = lane < head_dim
    inside = lax.broadcasted_iota(jnp.int32, (span, LANES), 0) < valid
    nt = (((1,), (1,)), ((), ()))

    def one_pair(p, cols):
        h = 2 * p
        xp = x_ref[:, pl.ds(p * LANES, LANES)]
        yp = dy_ref[:, pl.ds(p * LANES, LANES)]
        outs = []
        sums = None
        for j in range(2):
            scores = lax.dot_general(
                xp * (keep1 if j else keep0), yp, nt, preferred_element_type=F32
            )
            row = row_ref[pl.ds(step * per_step + h + j, 1), :]
            col = cols[:, h + j : h + j + 1]
            f00 = jnp.exp2(jnp.minimum(row[:, :half] - col[:half], 100.0))
            f01 = jnp.exp2(row[:, half:] - col[:half])
            f11 = jnp.exp2(jnp.minimum(row[:, half:] - col[half:], 100.0))
            k00 = (f00 * cb_ref[:half, :half]).astype(BF16)
            k01 = (f01 * cb_ref[:half, half:]).astype(BF16)
            k11 = (f11 * cb_ref[half:, half:]).astype(BF16)
            top = jnp.dot(
                jnp.concatenate([k00, k01], axis=1), yp, preferred_element_type=F32
            )
            bottom = jnp.dot(k11, yp[half:], preferred_element_type=F32)
            outs.append(jnp.concatenate([top, bottom], axis=0))
            terms = [
                f00 * scores[:half, :half],
                f01 * scores[:half, half:],
                f11 * scores[half:, half:],
            ]
            sums = terms if sums is None else [a + b for a, b in zip(sums, terms)]
        mix_ref[:half, :half] += sums[0]
        mix_ref[:half, half:] += sums[1]
        mix_ref[half:, half:] += sums[2]
        at = head0 + step * per_step + h
        skip = jnp.where(low, skip_ref[at], skip_ref[at + 1])
        direct = jnp.where(inside, skip * yp.astype(F32), 0.0)
        part_ref[:, pl.ds(p * LANES, LANES)] = (
            jnp.where(low, outs[0], outs[1]) + direct
        ).astype(part_ref.dtype)

    if call_heads == per_step:
        cols = col_ref[...]
    else:
        cols = jnp.where(step == 0, col_ref[:, :per_step], col_ref[:, per_step:])
    for p in range(per_step // 2):
        one_pair(p, cols)


def intra(head0, call_heads, per_step, length, skip, ld, dt, b, c, x, dy, mix, part):
    heads, span = ld.shape
    columns = x.shape[1]
    head_dim = columns // heads
    first = mix is None
    width = per_step * head_dim
    base = head0 // per_step
    whole = lambda: pl.BlockSpec(memory_space=VM)
    slab = lambda: pl.BlockSpec((span, width), lambda i: (0, base + i))
    smem = lambda: pl.BlockSpec(memory_space=pltpu.SMEM)
    in_specs = [smem(), smem()] + [whole() for _ in range(4)] + [slab(), slab()]
    args = [length, skip, ld, dt, b, c, x, dy]
    aliases = {}
    if not first:
        in_specs += [whole(), pl.BlockSpec(memory_space=ANY)]
        args += [mix, part]
        aliases = {9: 0}
    return pl.pallas_call(
        functools.partial(intra_kernel, head0, per_step, head_dim, first),
        grid=(call_heads // per_step,),
        out_shape=[
            jax.ShapeDtypeStruct((span, columns), BF16),
            jax.ShapeDtypeStruct((span, span), F32),
        ],
        in_specs=in_specs,
        out_specs=[slab(), pl.BlockSpec((span, span), lambda i: (0, 0))],
        scratch_shapes=[
            pltpu.VMEM((span, span), F32),
            pltpu.VMEM((call_heads, span), F32),
            pltpu.VMEM((span, call_heads), F32),
        ],
        input_output_aliases=aliases,
        compiler_params=pltpu.CompilerParams(vmem_limit_bytes=24 << 20),
        cost_estimate=pl.CostEstimate(
            flops=call_heads * 2 * 2 * span * span * 256,
            transcendentals=call_heads * span * span,
            bytes_accessed=call_heads * head_dim * span * 2 * 3,
        ),
        name="intra",
    )(*args)


def inter_kernel(
    own, last, head_dim, scale_b, scale_c, len_ref, ld_ref, dt_ref, b_ref, c_ref,
    x_ref, dy_ref, one_ref, two_ref, gb_in, gc_in, part_ref, out_ref, gb_ref, gc_ref, ws_ref, wg_ref
):
    idx, mine, lower = place()
    half = mine if own else 1 - mine
    span, width = x_ref.shape
    heads = ld_ref.shape[0]
    half_heads = heads // 2
    states = b_ref.shape[0]
    valid = valid_rows(len_ref, span)
    step = pl.program_id(0)
    nt = (((1,), (1,)), ((), ()))

    @pl.when(step == 0)
    def _():
        rows = pl.ds(pl.multiple_of(half * half_heads, 8), half_heads)
        end, into_state, into_grad = weights(ld_ref[rows, :], dt_ref[rows, :], valid)
        ws_ref[...] = into_state
        wg_ref[...] = into_grad
        if last:
            gb_ref[...] = gb_in[...]
            gc_ref[...] = gc_in[...]
        else:
            t = lax.broadcasted_iota(jnp.int32, (span, span), 0)
            u = lax.broadcasted_iota(jnp.int32, (span, span), 1)
            mix = jnp.where(jnp.logical_and(u >= t, u < valid), gb_in[...], 0.0)
            high = mix.astype(BF16)
            rest = (mix - high.astype(F32)).astype(BF16)
            c = c_ref[...]
            b = b_ref[...]
            gb_ref[...] = lax.dot_general(
                c, high, nt, preferred_element_type=F32
            ) + lax.dot_general(c, rest, nt, preferred_element_type=F32)
            gc_ref[...] = jnp.dot(b, high, preferred_element_type=F32) + jnp.dot(
                b, rest, preferred_element_type=F32
            )

    per = 2 * LANES // head_dim
    slab = 2 * LANES
    rowhead = lax.broadcasted_iota(jnp.int32, (per * states, slab), 0) // states
    lanehead = lax.broadcasted_iota(jnp.int32, (per * states, slab), 1) // head_dim
    diag = (rowhead == lanehead).astype(F32).astype(BF16)
    b = b_ref[...].astype(F32)
    groups = width // slab
    gb = None
    gc = None
    for g in range(groups):
        tile = step * (2 * groups) + 2 * g
        a0, a1 = one_ref[tile], one_ref[tile + 1]
        z0, z1 = two_ref[tile], two_ref[tile + 1]
        one = jnp.concatenate([a0, a1], axis=1)
        two = jnp.concatenate([z0, z1], axis=1)
        grad = jnp.where(lower, two, one)
        state = jnp.where(lower, one, two)
        grad_diag = jnp.concatenate([grad] * per, axis=0) * diag
        state_diag = jnp.concatenate([state] * per, axis=0) * diag
        h = step * (groups * per) + g * per
        rows_s = [ws_ref[pl.ds(h + j, 1), :] for j in range(per)]
        rows_g = [wg_ref[pl.ds(h + j, 1), :] for j in range(per)]
        left = jnp.concatenate([(b * r).astype(BF16) for r in rows_s], axis=0)
        cols = pl.ds(g * slab, slab)
        across = lax.dot_general(
            left, grad_diag, (((0,), (0,)), ((), ())), preferred_element_type=F32
        )
        out_ref[:, cols] = (part_ref[:, cols].astype(F32) + across).astype(out_ref.dtype)
        rb = lax.dot_general(grad_diag, x_ref[:, cols], nt, preferred_element_type=F32)
        rc = lax.dot_general(state_diag, dy_ref[:, cols], nt, preferred_element_type=F32)
        for j in range(per):
            tb = rows_s[j] * rb[j * states : (j + 1) * states]
            tc = rows_g[j] * rc[j * states : (j + 1) * states]
            gb = tb if gb is None else gb + tb
            gc = tc if gc is None else gc + tc
    gb_ref[...] += gb
    gc_ref[...] += gc
    if last:

        @pl.when(step == pl.num_programs(0) - 1)
        def _():
            gb_ref[...] = gb_ref[...] * scale_b
            gc_ref[...] = gc_ref[...] * scale_c


def inter(own, last, scale_b, scale_c, length, ld, dt, b, c, x, dy, one, two, gb, gc, part):
    heads, span = ld.shape
    columns = x.shape[1]
    head_dim = columns // heads
    states = b.shape[0]
    steps = 3
    width = columns // 2 // steps
    whole = lambda: pl.BlockSpec(memory_space=VM)

    def at(i):
        mine = lax.rem(lax.axis_index("seq"), 2)
        return (0, (mine if own else 1 - mine) * steps + i)

    slab = lambda: pl.BlockSpec((span, width), at)
    small = jax.ShapeDtypeStruct((states, span), F32)
    return pl.pallas_call(
        functools.partial(inter_kernel, own, last, head_dim, scale_b, scale_c),
        grid=(steps,),
        out_shape=[jax.ShapeDtypeStruct((span, columns), BF16), small, small],
        in_specs=[pl.BlockSpec(memory_space=pltpu.SMEM)]
        + [whole() for _ in range(4)]
        + [slab(), slab()]
        + [whole() for _ in range(4)]
        + [slab()],
        out_specs=[slab(), pl.BlockSpec((states, span), lambda i: (0, 0))]
        + [pl.BlockSpec((states, span), lambda i: (0, 0))],
        scratch_shapes=[pltpu.VMEM((heads // 2, span), F32)] * 2,
        input_output_aliases={11: 0},
        compiler_params=pltpu.CompilerParams(vmem_limit_bytes=24 << 20),
        cost_estimate=pl.CostEstimate(
            flops=heads // 2 * 2 * span * span * 256,
            transcendentals=0,
            bytes_accessed=columns // 2 * span * 2 * 4,
        ),
        name="inter",
    )(length, ld, dt, b, c, x, dy, one, two, gb, gc, part)


def local(inputs, out_grad, step_size, log_decay, b_matrix, c_matrix, skip_gain, lengths):
    x, dy, dt, ld = inputs[0], out_grad[0], step_size[0], log_decay[0]
    b, c = b_matrix[0], c_matrix[0]
    tokens, columns = x.shape
    heads = ld.shape[0]
    states = b.shape[0]
    count = lax.axis_size("seq")
    units = count // 2
    if tokens != SPAN or count % 4:
        raise ValueError("unsupported sizes")
    scale_b = 1.0 / math.sqrt(columns)
    scale_c = math.sqrt(states / (columns * count * tokens))
    swap = lambda v: lax.ppermute(v, "seq", [(i, i ^ 1) for i in range(count)])

    def hop(v, s):
        back = units - 1 - s
        pairs = [(2 * s + q, 2 * (s + 1) + q) for q in range(2)]
        pairs += [(2 * back + q, 2 * (back - 1) + q) for q in range(2)]
        return lax.ppermute(v, "seq", pairs)

    small = (ld, dt, b, c, x, dy)
    x1_send, d_send = summary(((True, False),), (BF16,), lengths, *small)
    y1, d_other = swap((x1_send, d_send))
    x2_own, x1_own, x2_send, d_own = summary(
        ((False, True), (True, True), (False, False)), (F32, F32, BF16), lengths, *small
    )
    y2 = swap(x2_send)

    received = []
    for s in range(units - 1):
        near = s < units // 2
        args = (d_other, d_own, x1_own, y1) if near else (d_other, d_own, x2_own, y2)
        (msg,) = chain(not near, *args, received[-1:], True, False)
        received.append(hop(msg, s))
    early = received[: units // 2 - 1]
    late = received[units // 2 - 1 :]
    own1, send1 = chain(False, d_other, d_own, x1_own, y1, early, False, True)
    got1 = swap(send1)
    own2, send2 = chain(True, d_other, d_own, x2_own, y2, late, False, True)
    got2 = swap(send2)

    mix = part = None
    call_heads = 16
    for head0 in range(0, heads, call_heads):
        part, mix = intra(
            head0, call_heads, 8, lengths, skip_gain, ld, dt, b, c, x, dy, mix, part
        )
    part, gb, gc = inter(
        True, False, scale_b, scale_c, lengths, *small, own1, own2, mix, mix, part
    )
    part, gb, gc = inter(
        False, True, scale_b, scale_c, lengths, *small, got1, got2, gb, gc, part
    )
    return (part[None], gb[None], gc[None])


def solution(mesh):
    placed = (
        P("batch", "seq", None),
        P("batch", "seq", None),
        P("batch", None, "seq"),
        P("batch", None, "seq"),
        P("batch", None, "seq"),
        P("batch", None, "seq"),
        P(),
        P("batch"),
    )
    return jax.shard_map(
        local,
        mesh=mesh,
        in_specs=placed,
        out_specs=(P("batch", "seq", None), P("batch", None, "seq"), P("batch", None, "seq")),
        check_vma=False,
    )
```

```python
import functools
import math

import jax
import jax.numpy as jnp
from jax import lax
from jax.experimental import pallas as pl
from jax.experimental.pallas import tpu as pltpu
from jax.sharding import PartitionSpec as P

SPAN = 256
LANES = 128
SLAB = 2 * LANES
LOG2E = math.log2(math.e)
F32 = jnp.float32
BF16 = jnp.bfloat16
NT = (((1,), (1,)), ((), ()))
TN = (((0,), (0,)), ((), ()))
OTHER, OWN = 0, 1


def place():
    idx = lax.axis_index("seq")
    count = lax.axis_size("seq")
    return idx, lax.rem(idx, 2), idx < count // 2


def mm(a, b, dims=None):
    if dims is None:
        return jnp.dot(a, b, preferred_element_type=F32)
    return lax.dot_general(a, b, dims, preferred_element_type=F32)


def whole():
    return pl.BlockSpec(memory_space=pltpu.VMEM)


def smem():
    return pl.BlockSpec(memory_space=pltpu.SMEM)


def hbm():
    return pl.BlockSpec(memory_space=pltpu.HBM)


def iota(shape, axis):
    return lax.broadcasted_iota(jnp.int32, shape, axis)


def running_sum(values):
    rows, span = values.shape
    sub = span // 2
    high = values.astype(BF16)
    rest = values - high.astype(F32)
    middle = rest.astype(BF16)
    low = (rest - middle.astype(F32)).astype(BF16)
    upper = (iota((sub, sub), 0) <= iota((sub, sub), 1)).astype(F32).astype(BF16)
    pieces = jnp.concatenate([high, middle, low], axis=0)
    halves = []
    for s in range(2):
        sums = mm(pieces[:, s * sub : (s + 1) * sub], upper)
        halves.append(sums[:rows] + sums[rows : 2 * rows] + sums[2 * rows :])
    return jnp.concatenate(halves, axis=1)


def weights(ld, dt):
    cum = running_sum(ld)
    rows, span = cum.shape
    sub = span // 2
    end_a, end_b = cum[:, sub - 1 : sub], cum[:, span - 1 : span]
    ends = jnp.where(iota(cum.shape, 1) < sub, end_a, end_b)
    return cum, dt * jnp.exp(ends - cum), jnp.exp(cum), jnp.exp(end_a), jnp.exp(end_b)


def spread(column, scratch_ref, head_dim):
    rows = scratch_ref.shape[0]
    scratch_ref[...] = jnp.broadcast_to(column, scratch_ref.shape)
    even = scratch_ref[pl.ds(0, rows // 2, stride=2), :]
    odd = scratch_ref[pl.ds(1, rows // 2, stride=2), :]
    return jnp.where(iota(even.shape, 1) < head_dim, even, odd)


def load_tasks(tasks, kinds, mine, x_ref, dy_ref, data_ref, sems):
    width = data_ref.shape[3]
    chunks = sems.shape[1]
    chunk = width // chunks

    def copy(t, i, kind, src):
        rel = OWN if tasks[t][1] else OTHER
        half = mine if tasks[t][1] else 1 - mine
        start = pl.multiple_of(half * width + i * chunk, LANES)
        return pltpu.make_async_copy(
            src.at[:, pl.ds(start, chunk)],
            data_ref.at[rel, kind, :, pl.ds(i * chunk, chunk)],
            sems.at[t, i],
        )

    for t in range(len(tasks)):
        for i in range(chunks):

            @pl.when(kinds[t] == 0)
            def _():
                copy(t, i, 0, x_ref).start()

            @pl.when(kinds[t] == 1)
            def _():
                copy(t, i, 1, dy_ref).start()

    return lambda t, i: copy(t, i, kinds[t], x_ref).wait()


def run_task(t, kind, rel, valid, wait, chunks, head_dim, b, c, w_ref, rows_ref, data_ref, x_ref, sub_ref):
    span, width = data_ref.shape[2:]
    half_span = span // 2
    chunk = width // chunks
    is_state = kind == 0
    mat = jnp.where(is_state, b, c)
    states = mat.shape[0]
    per = SLAB // head_dim
    low = iota((states, LANES), 1) < head_dim
    for i in range(chunks):
        wait(t, i)

        @pl.when(jnp.logical_and(kind == 1, valid < span))
        def _():
            cols = pl.ds(i * chunk, chunk)
            inside = iota((span, chunk), 0) < valid
            data = data_ref[rel, 1, :, cols].astype(F32)
            data_ref[rel, 1, :, cols] = jnp.where(inside, data, 0.0).astype(BF16)

        for g in range(i * chunk // SLAB, (i + 1) * chunk // SLAB):
            lhs = jnp.concatenate(
                [(mat * w_ref[pl.ds(per * g + j, 1), :]).astype(BF16) for j in range(per)],
                axis=0,
            )
            cols = pl.ds(SLAB * g, SLAB)
            parts = [
                mm(
                    lhs[:, s * half_span : (s + 1) * half_span],
                    data_ref[rel, kind, pl.ds(s * half_span, half_span), cols],
                )
                for s in range(2)
            ]
            for q in range(2):
                lanes = slice(q * LANES, (q + 1) * LANES)
                top = slice(2 * q * states, (2 * q + 1) * states)
                bottom = slice((2 * q + 1) * states, (2 * q + 2) * states)
                e0, e1 = [jnp.where(low, p[top, lanes], p[bottom, lanes]) for p in parts]
                j = 2 * g + q
                d_a, d_b = rows_ref[0, pl.ds(j, 1), :], rows_ref[1, pl.ds(j, 1), :]
                total = jnp.where(is_state, d_b, 1.0) * e0 + jnp.where(is_state, 1.0, d_a) * e1
                x_ref[j] = total.astype(x_ref.dtype)
                sub_ref[j] = jnp.where(is_state, e0, e1)


def first_kernel(
    head_dim, len_ref, ld_hbm, dt_hbm, b_hbm, c_hbm, x_ref, dy_ref,
    msg_ref, sub_ref, data_ref, ld_ref, dt_ref, b_ref, c_ref, w_ref, rows_ref, spread_ref, sems, small_sems
):
    idx, mine, lower = place()
    kind = jnp.where(lower, 0, 1)
    span = ld_ref.shape[1]
    half_heads = ld_ref.shape[0] // 2
    small = [
        pltpu.make_async_copy(src, dst, small_sems.at[i])
        for i, (src, dst) in enumerate(
            ((ld_hbm, ld_ref), (dt_hbm, dt_ref), (b_hbm, b_ref), (c_hbm, c_ref))
        )
    ]
    for copy in small:
        copy.start()
    wait = load_tasks(((True, False),), (kind,), mine, x_ref, dy_ref, data_ref, sems)
    for copy in small:
        copy.wait()
    rows = pl.ds(pl.multiple_of((1 - mine) * half_heads, 8), half_heads)
    cum, ws, wg, d_a, d_b = weights(ld_ref[rows, :], dt_ref[rows, :])
    w_ref[...] = jnp.where(kind == 0, ws, wg)
    rows_a = spread(d_a, spread_ref, head_dim)
    rows_b = spread(d_b, spread_ref, head_dim)
    rows_ref[0] = rows_a
    rows_ref[1] = rows_b
    both = rows_a * rows_b
    high = both.astype(BF16).astype(F32)
    tiles = sub_ref.shape[0]
    extra = jnp.concatenate([high, both - high], axis=0).astype(BF16)
    msg_ref[tiles:] = extra.reshape((msg_ref.shape[0] - tiles,) + msg_ref.shape[1:])
    valid = len_ref[0] - idx * span
    run_task(
        0, kind, OTHER, valid, wait, sems.shape[1], head_dim,
        b_ref[...].astype(F32), c_ref[...].astype(F32), w_ref, rows_ref, data_ref, msg_ref, sub_ref,
    )


def first_part(length, ld, dt, b, c, x, dy):
    heads, span = ld.shape
    columns = x.shape[1]
    states = b.shape[0]
    tiles = columns // 2 // LANES
    pairs = heads // 4
    tile = lambda n, t: jax.ShapeDtypeStruct((n, states, LANES), t)
    same = lambda a: jax.ShapeDtypeStruct(a.shape, a.dtype)
    return pl.pallas_call(
        functools.partial(first_kernel, columns // heads),
        out_shape=[
            tile(tiles + 2 * pairs // states, BF16),
            tile(tiles, F32),
            jax.ShapeDtypeStruct((2, 2, span, columns // 2), BF16),
            same(ld), same(dt), same(b), same(c),
        ],
        in_specs=[smem()] + [hbm() for _ in range(6)],
        out_specs=[whole() for _ in range(7)],
        scratch_shapes=[
            pltpu.VMEM((heads // 2, span), F32),
            pltpu.VMEM((2, pairs, LANES), F32),
            pltpu.VMEM((heads // 2, LANES), F32),
            pltpu.SemaphoreType.DMA((1, 4)),
            pltpu.SemaphoreType.DMA((4,)),
        ],
        compiler_params=pltpu.CompilerParams(vmem_limit_bytes=12 << 20),
        name="first",
    )(length, ld, dt, b, c, x, dy)


def rest_kernel(
    head_dim, len_ref, skip_ref, ld_ref, dt_ref, b_ref, c_ref, data_in, x_ref, dy_ref,
    data_ref, send_ref, x1_ref, x2_ref, sub_other_ref, sub1_ref, sub2_ref, d_ref, rows_ref,
    w_ref, row_ref, col_ref, cb_ref, skip_rows_ref, task_w_ref, spread_ref, sems
):
    idx, mine, lower = place()
    kind1 = jnp.where(lower, 0, 1)
    kind2 = 1 - kind1
    heads, span = ld_ref.shape
    half_heads = heads // 2
    pairs = half_heads // 2
    sub = span // 2
    tasks = ((True, True), (False, True), (False, False))
    kinds = (kind1, kind2, kind2)
    wait = load_tasks(tasks, kinds, mine, x_ref, dy_ref, data_ref, sems)
    low = iota((1, LANES), 1) < head_dim
    for rel in (OTHER, OWN):
        half = mine if rel == OWN else 1 - mine
        rows = pl.ds(pl.multiple_of(half * half_heads, 8), half_heads)
        dt = dt_ref[rows, :]
        cum, ws, wg, d_a, d_b = weights(ld_ref[rows, :], dt)
        w_ref[rel, 0] = ws
        w_ref[rel, 1] = wg
        rows_ref[rel, 0] = spread(d_a, spread_ref, head_dim)
        rows_ref[rel, 1] = spread(d_b, spread_ref, head_dim)
        row = cum * LOG2E
        row_ref[rel] = row
        col_ref[rel] = (row - jnp.log(dt) * LOG2E).T
        for j in range(pairs):
            at = half * half_heads + 2 * j
            skip_rows_ref[rel, pl.ds(j, 1), :] = jnp.where(low, skip_ref[at], skip_ref[at + 1])
    d_ref[...] = rows_ref[OWN, 0] * rows_ref[OWN, 1]
    for s in range(2):
        cols = slice(s * sub, (s + 1) * sub)
        dots = mm(b_ref[:, cols], c_ref[:, cols], TN)
        cb_ref[s] = jnp.where(iota(dots.shape, 1) >= iota(dots.shape, 0), dots, 0.0)
    b, c = b_ref[...].astype(F32), c_ref[...].astype(F32)
    valid = len_ref[0] - idx * span
    outs = ((x1_ref, sub1_ref), (x2_ref, sub2_ref), (send_ref, sub_other_ref))
    for t, (first, own) in enumerate(tasks):
        rel = OWN if own else OTHER
        task_w_ref[t] = jnp.where(kinds[t] == 0, w_ref[rel, 0], w_ref[rel, 1])
        run_task(
            t, kinds[t], rel, valid, wait, sems.shape[1], head_dim, b, c,
            task_w_ref.at[t], rows_ref.at[rel], data_ref, outs[t][0], outs[t][1],
        )


def rest_part(length, skip, ld, dt, b, c, data, x, dy):
    heads, span = ld.shape
    columns = x.shape[1]
    states = b.shape[0]
    tiles = columns // 2 // LANES
    pairs = heads // 4
    sub = span // 2
    shape = jax.ShapeDtypeStruct
    tile = lambda t: shape((tiles, states, LANES), t)
    outs = [
        shape(data.shape, BF16),
        tile(BF16), tile(F32), tile(F32), tile(F32), tile(F32), tile(F32),
        shape((pairs, LANES), F32),
        shape((2, 2, pairs, LANES), F32),
        shape((2, 2, heads // 2, span), F32),
        shape((2, heads // 2, span), F32),
        shape((2, span, heads // 2), F32),
        shape((2, sub, sub), F32),
        shape((2, pairs, LANES), F32),
    ]
    return pl.pallas_call(
        functools.partial(rest_kernel, columns // heads),
        out_shape=outs,
        in_specs=[smem(), smem()] + [whole() for _ in range(5)] + [hbm(), hbm()],
        out_specs=[whole() for _ in outs],
        scratch_shapes=[
            pltpu.VMEM((3, heads // 2, span), F32),
            pltpu.VMEM((heads // 2, LANES), F32),
            pltpu.SemaphoreType.DMA((3, 4)),
        ],
        input_output_aliases={6: 0},
        compiler_params=pltpu.CompilerParams(vmem_limit_bytes=16 << 20),
        name="rest",
    )(length, skip, ld, dt, b, c, data, x, dy)


def pair_flags(second):
    idx, mine, lower = place()
    ahead = jnp.where(lower, mine == 0, mine == 1)
    return jnp.logical_not(ahead) if second else ahead


def chain_kernel(second, carries, finish, msg, *refs):
    decay_ref, mine_ref, x_ref, y_ref = refs[:4]
    carry_refs = refs[4 : 4 + carries]
    rest = refs[4 + carries :]
    dp_ref = rest[-1]
    ahead = pair_flags(second)
    tiles = x_ref.shape[0]
    count = dp_ref.shape[0]
    both = decay_ref[tiles:].reshape(2 * count, LANES).astype(F32)
    dp_ref[...] = both[:count] + both[count:]
    for j in range(tiles):
        dp = dp_ref[pl.ds(j, 1), :]
        d = mine_ref[pl.ds(j, 1), :]
        x = x_ref[j]
        y = y_ref[j].astype(F32)
        carry = None
        for ref in carry_refs:
            carry = ref[j].astype(F32) if carry is None else carry + ref[j].astype(F32)
        at = 0
        if msg:
            total = jnp.where(ahead, dp, d) * jnp.where(ahead, x, y) + jnp.where(ahead, y, x)
            if carry is not None:
                total = total + d * dp * carry
            rest[at][j] = total.astype(BF16)
            at += 1
        if finish:
            if carry is None:
                carry = jnp.zeros_like(x)
            passed = jnp.where(ahead, d, dp) * carry + jnp.where(ahead, x, y)
            rest[at][j] = jnp.where(ahead, carry, passed).astype(BF16)
            rest[at + 1][j] = jnp.where(ahead, passed, carry).astype(BF16)


def chain(second, decay, mine, x, y, carries, msg, finish):
    shape = jax.ShapeDtypeStruct(x.shape, BF16)
    outs = int(msg) + 2 * int(finish)
    return pl.pallas_call(
        functools.partial(chain_kernel, second, len(carries), finish, msg),
        out_shape=[shape] * outs,
        in_specs=[whole() for _ in range(4 + len(carries))],
        out_specs=[whole() for _ in range(outs)],
        scratch_shapes=[pltpu.VMEM(mine.shape, F32)],
        compiler_params=pltpu.CompilerParams(vmem_limit_bytes=4 << 20),
        name="chain",
    )(decay, mine, x, y, *carries)


def intra_kernel(rel, pair0, pairs, head_dim, first, row_ref, col_ref, cb_ref, skip_ref, data_ref, *refs):
    mix_in = None if first else refs[0]
    part_ref, mix_ref = refs[-2:]
    sub = cb_ref.shape[1]
    lane = iota((1, LANES), 1)
    keep = [
        (lane < head_dim).astype(F32).astype(BF16),
        (lane >= head_dim).astype(F32).astype(BF16),
    ]
    for s in range(2):
        here = pl.ds(s * sub, sub)
        acc = None if first else mix_in[s]
        for p in range(pairs):
            cols = pl.ds((pair0 + p) * LANES, LANES)
            xs = data_ref[rel, 0, here, cols]
            ys = data_ref[rel, 1, here, cols]
            split = jnp.concatenate([ys * keep[0], ys * keep[1]], axis=0)
            scores = mm(xs, split, NT)
            kernels = []
            for j in range(2):
                h = 2 * (pair0 + p) + j
                row = row_ref[rel, pl.ds(h, 1), here]
                col = col_ref[rel, here, pl.ds(h, 1)]
                decay = jnp.exp2(jnp.minimum(row - col, 100.0))
                kernels.append((decay * cb_ref[s]).astype(BF16))
                term = decay * scores[:, j * sub : (j + 1) * sub]
                acc = term if acc is None else acc + term
            within = mm(jnp.concatenate(kernels, axis=1), split)
            skip = skip_ref[rel, pl.ds(pair0 + p, 1), :]
            part_ref[here, pl.ds(p * LANES, LANES)] = (
                within + skip * ys.astype(F32)
            ).astype(part_ref.dtype)
        mix_ref[s] = acc


def intra(rel, pair0, pairs, head_dim, row, col, cb, skip, data, mix):
    span = data.shape[2]
    args = [row, col, cb, skip, data] + ([] if mix is None else [mix])
    heads = 2 * pairs
    return pl.pallas_call(
        functools.partial(intra_kernel, rel, pair0, pairs, head_dim, mix is None),
        out_shape=[
            jax.ShapeDtypeStruct((span, pairs * LANES), BF16),
            jax.ShapeDtypeStruct(cb.shape, F32),
        ],
        in_specs=[whole() for _ in args],
        out_specs=[whole(), whole()],
        compiler_params=pltpu.CompilerParams(vmem_limit_bytes=16 << 20),
        cost_estimate=pl.CostEstimate(
            flops=heads * 2 * span * span * 128,
            transcendentals=heads * span * span // 2,
            bytes_accessed=heads * head_dim * span * 2 * 3,
        ),
        name="intra",
    )(*args)


def inter_kernel(last, head_dim, slabs, scale_b, scale_c, b_ref, c_ref, w_ref, rows_ref, data_ref,
                 one_ref, two_ref, sub1_ref, sub2_ref, *refs):
    idx, mine, lower = place()
    rel = OTHER if last else OWN
    parts = refs[:slabs]
    refs = refs[slabs:]
    if last:
        gb_in, gc_in, slab_in, out_ref, gb_ref, gc_ref, buf_ref, sems = refs
    else:
        mix_ref, buf_ref, gb_ref, gc_ref = refs
    span, width = data_ref.shape[2:]
    sub = span // 2
    states = b_ref.shape[0]
    per = SLAB // head_dim
    if last:
        own_copy = pltpu.make_async_copy(
            slab_in, out_ref.at[:, pl.ds(pl.multiple_of(mine * width, LANES), width)], sems.at[0]
        )
        own_copy.start()
    rowhead = iota((per * states, SLAB), 0) // states
    lanehead = iota((per * states, SLAB), 1) // head_dim
    diag = (rowhead == lanehead).astype(F32).astype(BF16)
    b = b_ref[...].astype(F32)
    groups = width // SLAB
    slab_width = width // slabs
    gb = [None, None]
    gc = [None, None]
    copies = []
    sends = 1 if not last else sems.shape[0] - 1
    for g in range(groups):
        j = 2 * g
        pair = lambda ref: jnp.concatenate([ref[j], ref[j + 1]], axis=1)
        one, two, sub1, sub2 = pair(one_ref), pair(two_ref), pair(sub1_ref), pair(sub2_ref)
        grad = jnp.where(lower, two, one)
        state = jnp.where(lower, one, two)
        grad_sub = jnp.where(lower, sub2, sub1)
        state_sub = jnp.where(lower, sub1, sub2)
        row = lambda k: jnp.concatenate(
            [rows_ref[rel, k, pl.ds(j, 1), :], rows_ref[rel, k, pl.ds(j + 1, 1), :]], axis=1
        )
        grads = [(grad_sub + row(1) * grad.astype(F32)).astype(BF16), grad]
        states_in = [state, (state_sub + row(0) * state.astype(F32)).astype(BF16)]
        cols = pl.ds(g * SLAB, SLAB)
        part = parts[g * SLAB // slab_width]
        part_cols = pl.ds(g * SLAB % slab_width, SLAB)
        for s in range(2):
            here = pl.ds(s * sub, sub)
            rows_s = [w_ref[rel, 0, pl.ds(per * g + i, 1), here] for i in range(per)]
            rows_g = [w_ref[rel, 1, pl.ds(per * g + i, 1), here] for i in range(per)]
            grad_diag = jnp.concatenate([grads[s]] * per, axis=0) * diag
            state_diag = jnp.concatenate([states_in[s]] * per, axis=0) * diag
            bs = b[:, s * sub : (s + 1) * sub]
            left = jnp.concatenate([(bs * r).astype(BF16) for r in rows_s], axis=0)
            across = mm(left, grad_diag, TN)
            buf_ref[here, cols] = (part[here, part_cols].astype(F32) + across).astype(BF16)
            rb = mm(grad_diag, data_ref[rel, 0, here, cols], NT)
            rc = mm(state_diag, data_ref[rel, 1, here, cols], NT)
            for i in range(per):
                rows = slice(i * states, (i + 1) * states)
                tb, tc = rows_s[i] * rb[rows], rows_g[i] * rc[rows]
                gb[s] = tb if gb[s] is None else gb[s] + tb
                gc[s] = tc if gc[s] is None else gc[s] + tc
        if last and (g + 1) % (groups // sends) == 0:
            k = (g + 1) // (groups // sends) - 1
            wide = width // sends
            start = pl.multiple_of((1 - mine) * width + k * wide, LANES)
            send = pltpu.make_async_copy(
                buf_ref.at[:, pl.ds(k * wide, wide)],
                out_ref.at[:, pl.ds(start, wide)],
                sems.at[k + 1],
            )
            send.start()
            copies.append(send)
    gb = jnp.concatenate(gb, axis=1)
    gc = jnp.concatenate(gc, axis=1)
    if last:
        gb_ref[...] = (gb_in[...] + gb) * scale_b
        gc_ref[...] = (gc_in[...] + gc) * scale_c
        own_copy.wait()
        for send in copies:
            send.wait()
    else:
        mixed_b, mixed_c = [], []
        for s in range(2):
            here = slice(s * sub, (s + 1) * sub)
            keep = iota((sub, sub), 1) >= iota((sub, sub), 0)
            mix = jnp.where(keep, mix_ref[s], 0.0)
            high = mix.astype(BF16)
            rest = (mix - high.astype(F32)).astype(BF16)
            bs, cs = b_ref[:, here], c_ref[:, here]
            mixed_b.append(mm(cs, high, NT) + mm(cs, rest, NT))
            mixed_c.append(mm(bs, high) + mm(bs, rest))
        gb_ref[...] = gb + jnp.concatenate(mixed_b, axis=1)
        gc_ref[...] = gc + jnp.concatenate(mixed_c, axis=1)


def inter(last, head_dim, scale_b, scale_c, b, c, w, rows, data, one, two, sub1, sub2, parts, extra):
    states = b.shape[0]
    span, width = data.shape[2:]
    small = jax.ShapeDtypeStruct((states, span), F32)
    args = [b, c, w, rows, data, one, two, sub1, sub2, *parts, *extra]
    sends = 4
    if last:
        out0, spec0 = jax.ShapeDtypeStruct((span, 2 * width), BF16), hbm()
        scratch = [pltpu.VMEM((span, width), BF16), pltpu.SemaphoreType.DMA((sends + 1,))]
    else:
        out0, spec0 = jax.ShapeDtypeStruct((span, width), BF16), whole()
        scratch = []
    return pl.pallas_call(
        functools.partial(inter_kernel, last, head_dim, len(parts), scale_b, scale_c),
        out_shape=[out0, small, small],
        in_specs=[whole() for _ in args],
        out_specs=[spec0, whole(), whole()],
        scratch_shapes=scratch,
        compiler_params=pltpu.CompilerParams(vmem_limit_bytes=16 << 20),
        cost_estimate=pl.CostEstimate(
            flops=width * 2 * span * 256 * 3,
            transcendentals=0,
            bytes_accessed=width * span * 2 * 4,
        ),
        name="inter",
    )(*args)


def local(inputs, out_grad, step_size, log_decay, b_matrix, c_matrix, skip_gain, lengths):
    x, dy = inputs[0], out_grad[0]
    tokens, columns = x.shape
    heads = step_size.shape[1]
    states = b_matrix.shape[1]
    head_dim = columns // heads
    count = lax.axis_size("seq")
    units = count // 2
    if tokens != SPAN or count % 4:
        raise ValueError("unsupported sizes")
    scale_b = 1.0 / math.sqrt(columns)
    scale_c = math.sqrt(states / (columns * count * tokens))
    swap = lambda v: lax.ppermute(v, "seq", [(i, i ^ 1) for i in range(count)])

    def hop(v, s):
        back = units - 1 - s
        pairs = [(2 * s + q, 2 * (s + 1) + q) for q in range(2)]
        pairs += [(2 * back + q, 2 * (back - 1) + q) for q in range(2)]
        return lax.ppermute(v, "seq", pairs)

    fixed = lambda v: pltpu.with_memory_space_constraint(v, pltpu.HBM)
    x, dy = fixed(x), fixed(dy)
    small = [fixed(v) for v in (log_decay[0], step_size[0], b_matrix[0], c_matrix[0])]
    msg1, sub1_other, data, ld, dt, b, c = first_part(lengths, *small, x, dy)
    y1 = swap(msg1)
    data, x2_send, x1, x2, sub2_other, sub1, sub2, d, rows, w, row, col, cb, skip = rest_part(
        lengths, skip_gain, ld, dt, b, c, data, x, dy
    )
    y2 = swap(x2_send)

    received = []
    for s in range(units - 1):
        near = s < units // 2
        args = (y1, d, x1, y1) if near else (y1, d, x2, y2)
        (msg,) = chain(not near, *args, received[-1:], True, False)
        received.append(hop(msg, s))
    early = received[: units // 2 - 1]
    late = received[units // 2 - 1 :]
    own1, send1 = chain(False, y1, d, x1, y1, early, False, True)
    got1 = swap(send1)
    own2, send2 = chain(True, y1, d, x2, y2, late, False, True)
    got2 = swap(send2)

    calls = 3
    pairs = heads // 4 // calls
    mix = None
    parts = {OTHER: [], OWN: []}
    for rel in (OWN, OTHER):
        for k in range(calls):
            part, mix = intra(rel, k * pairs, pairs, head_dim, row, col, cb, skip, data, mix)
            parts[rel].append(part)
    slab, gb, gc = inter(
        False, head_dim, scale_b, scale_c, b, c, w, rows, data, own1, own2, sub1, sub2,
        parts[OWN], [mix],
    )
    out, gb, gc = inter(
        True, head_dim, scale_b, scale_c, b, c, w, rows, data, got1, got2, sub1_other, sub2_other,
        parts[OTHER], [gb, gc, slab],
    )
    return (out[None], gb[None], gc[None])


def solution(mesh):
    placed = (
        P("batch", "seq", None),
        P("batch", "seq", None),
        P("batch", None, "seq"),
        P("batch", None, "seq"),
        P("batch", None, "seq"),
        P("batch", None, "seq"),
        P(),
        P("batch"),
    )
    return jax.shard_map(
        local,
        mesh=mesh,
        in_specs=placed,
        out_specs=(P("batch", "seq", None), P("batch", None, "seq"), P("batch", None, "seq")),
        check_vma=False,
    )
```

```python
import functools
import math

import jax
import jax.numpy as jnp
from jax import lax
from jax.experimental import pallas as pl
from jax.experimental.pallas import tpu as pltpu
from jax.sharding import PartitionSpec as P

SPAN = 256
LANES = 128
SLAB = 2 * LANES
LOG2E = math.log2(math.e)
F32 = jnp.float32
BF16 = jnp.bfloat16
NT = (((1,), (1,)), ((), ()))
TN = (((0,), (0,)), ((), ()))
OTHER, OWN = 0, 1


def place():
    idx = lax.axis_index("seq")
    count = lax.axis_size("seq")
    return idx, lax.rem(idx, 2), idx < count // 2


def mm(a, b, dims=None):
    if dims is None:
        return jnp.dot(a, b, preferred_element_type=F32)
    return lax.dot_general(a, b, dims, preferred_element_type=F32)


def whole():
    return pl.BlockSpec(memory_space=pltpu.VMEM)


def smem():
    return pl.BlockSpec(memory_space=pltpu.SMEM)


def hbm():
    return pl.BlockSpec(memory_space=pltpu.HBM)


def iota(shape, axis):
    return lax.broadcasted_iota(jnp.int32, shape, axis)


def running_sum(values):
    rows, span = values.shape
    sub = span // 2
    high = values.astype(BF16)
    rest = values - high.astype(F32)
    middle = rest.astype(BF16)
    low = (rest - middle.astype(F32)).astype(BF16)
    upper = (iota((sub, sub), 0) <= iota((sub, sub), 1)).astype(F32).astype(BF16)
    pieces = jnp.concatenate([high, middle, low], axis=0)
    halves = []
    for s in range(2):
        sums = mm(pieces[:, s * sub : (s + 1) * sub], upper)
        halves.append(sums[:rows] + sums[rows : 2 * rows] + sums[2 * rows :])
    return jnp.concatenate(halves, axis=1)


def weights(ld, dt):
    cum = running_sum(ld)
    rows, span = cum.shape
    sub = span // 2
    end_a, end_b = cum[:, sub - 1 : sub], cum[:, span - 1 : span]
    ends = jnp.where(iota(cum.shape, 1) < sub, end_a, end_b)
    return cum, dt * jnp.exp(ends - cum), jnp.exp(cum), jnp.exp(end_a), jnp.exp(end_b)


def spread(column, scratch_ref, head_dim):
    rows = scratch_ref.shape[0]
    scratch_ref[...] = jnp.broadcast_to(column, scratch_ref.shape)
    even = scratch_ref[pl.ds(0, rows // 2, stride=2), :]
    odd = scratch_ref[pl.ds(1, rows // 2, stride=2), :]
    return jnp.where(iota(even.shape, 1) < head_dim, even, odd)


def load_tasks(tasks, kinds, mine, x_ref, dy_ref, data_ref, sems):
    width = data_ref.shape[3]
    chunks = sems.shape[1]
    chunk = width // chunks

    def copy(t, i, kind, src):
        rel = OWN if tasks[t][1] else OTHER
        half = mine if tasks[t][1] else 1 - mine
        start = pl.multiple_of(half * width + i * chunk, LANES)
        return pltpu.make_async_copy(
            src.at[:, pl.ds(start, chunk)],
            data_ref.at[rel, kind, :, pl.ds(i * chunk, chunk)],
            sems.at[t, i],
        )

    for t in range(len(tasks)):
        for i in range(chunks):

            @pl.when(kinds[t] == 0)
            def _():
                copy(t, i, 0, x_ref).start()

            @pl.when(kinds[t] == 1)
            def _():
                copy(t, i, 1, dy_ref).start()

    return lambda t, i: copy(t, i, kinds[t], x_ref).wait()


def run_task(t, kind, rel, valid, wait, chunks, head_dim, b, c, w_ref, rows_ref, data_ref, x_ref, sub_ref):
    span, width = data_ref.shape[2:]
    half_span = span // 2
    chunk = width // chunks
    is_state = kind == 0
    mat = jnp.where(is_state, b, c)
    states = mat.shape[0]
    per = SLAB // head_dim
    low = iota((states, LANES), 1) < head_dim
    for i in range(chunks):
        if wait is not None:
            wait(t, i)
            mask_rows(rel, kind, valid, pl.ds(i * chunk, chunk), data_ref)
        for g in range(i * chunk // SLAB, (i + 1) * chunk // SLAB):
            lhs = jnp.concatenate(
                [(mat * w_ref[pl.ds(per * g + j, 1), :]).astype(BF16) for j in range(per)],
                axis=0,
            )
            cols = pl.ds(SLAB * g, SLAB)
            parts = [
                mm(
                    lhs[:, s * half_span : (s + 1) * half_span],
                    data_ref[rel, kind, pl.ds(s * half_span, half_span), cols],
                )
                for s in range(2)
            ]
            for q in range(2):
                lanes = slice(q * LANES, (q + 1) * LANES)
                top = slice(2 * q * states, (2 * q + 1) * states)
                bottom = slice((2 * q + 1) * states, (2 * q + 2) * states)
                e0, e1 = [jnp.where(low, p[top, lanes], p[bottom, lanes]) for p in parts]
                j = 2 * g + q
                d_a, d_b = rows_ref[0, pl.ds(j, 1), :], rows_ref[1, pl.ds(j, 1), :]
                total = jnp.where(is_state, d_b, 1.0) * e0 + jnp.where(is_state, 1.0, d_a) * e1
                x_ref[j] = total.astype(x_ref.dtype)
                sub_ref[j] = jnp.where(is_state, e0, e1)


def first_kernel(
    head_dim, len_ref, ld_hbm, dt_hbm, b_hbm, c_hbm, x_ref, dy_ref,
    msg_ref, sub1_ref, sub2_ref, data_ref, ld_ref, dt_ref, b_ref, c_ref, w_ref, rows_ref, row_ref,
    task_w_ref, spread_ref, sems, small_sems
):
    idx, mine, lower = place()
    kind1 = jnp.where(lower, 0, 1)
    kinds = (kind1, 1 - kind1)
    span = ld_ref.shape[1]
    half_heads = ld_ref.shape[0] // 2
    small = [
        pltpu.make_async_copy(src, dst, small_sems.at[i])
        for i, (src, dst) in enumerate(
            ((ld_hbm, ld_ref), (dt_hbm, dt_ref), (b_hbm, b_ref), (c_hbm, c_ref))
        )
    ]
    for copy in small:
        copy.start()
    wait = load_tasks(((True, False), (False, False)), kinds, mine, x_ref, dy_ref, data_ref, sems)
    for copy in small:
        copy.wait()
    rows = pl.ds(pl.multiple_of((1 - mine) * half_heads, 8), half_heads)
    cum, ws, wg, d_a, d_b = weights(ld_ref[rows, :], dt_ref[rows, :])
    w_ref[0] = ws
    w_ref[1] = wg
    row_ref[...] = cum * LOG2E
    rows_a = spread(d_a, spread_ref, head_dim)
    rows_b = spread(d_b, spread_ref, head_dim)
    rows_ref[0] = rows_a
    rows_ref[1] = rows_b
    tiles = sub1_ref.shape[0]
    extra = narrow_rows(rows_a * rows_b)
    msg_ref[2 * tiles :] = extra.reshape((msg_ref.shape[0] - 2 * tiles,) + msg_ref.shape[1:])
    valid = len_ref[0] - idx * span
    b, c = b_ref[...].astype(F32), c_ref[...].astype(F32)
    for t, sub_ref in enumerate((sub1_ref, sub2_ref)):
        task_w_ref[t] = jnp.where(kinds[t] == 0, ws, wg)
        run_task(
            t, kinds[t], OTHER, valid, wait, sems.shape[1], head_dim, b, c, task_w_ref.at[t],
            rows_ref, data_ref, msg_ref.at[pl.ds(t * tiles, tiles)], sub_ref,
        )


def first_part(length, ld, dt, b, c, x, dy):
    heads, span = ld.shape
    columns = x.shape[1]
    states = b.shape[0]
    tiles = columns // 2 // LANES
    pairs = heads // 4
    shape = jax.ShapeDtypeStruct
    tile = lambda n, t: shape((n, states, LANES), t)
    same = lambda a: shape(a.shape, a.dtype)
    outs = [
        tile(2 * tiles + 2 * pairs // states, BF16),
        tile(tiles, F32),
        tile(tiles, F32),
        shape((2, 2, span, columns // 2), BF16),
        same(ld), same(dt), same(b), same(c),
    ] + table_shapes(heads, span)[:3]
    return pl.pallas_call(
        functools.partial(first_kernel, columns // heads),
        out_shape=outs,
        in_specs=[smem()] + [hbm() for _ in range(6)],
        out_specs=[whole() for _ in outs],
        scratch_shapes=[
            pltpu.VMEM((2, heads // 2, span), F32),
            pltpu.VMEM((heads // 2, LANES), F32),
            pltpu.SemaphoreType.DMA((2, 4)),
            pltpu.SemaphoreType.DMA((4,)),
        ],
        compiler_params=pltpu.CompilerParams(vmem_limit_bytes=12 << 20),
        name="first",
    )(length, ld, dt, b, c, x, dy)


def mask_rows(rel, kind, valid, cols, data_ref):
    span = data_ref.shape[2]

    @pl.when(jnp.logical_and(kind == 1, valid < span))
    def _():
        inside = iota((span, cols.size), 0) < valid
        data = data_ref[rel, 1, :, cols].astype(F32)
        data_ref[rel, 1, :, cols] = jnp.where(inside, data, 0.0).astype(BF16)


def more_tables(half, head_dim, row, dt_ref, skip_ref, col_ref, skip_rows_ref):
    half_heads = row.shape[0]
    low = iota((1, LANES), 1) < head_dim
    rows = pl.ds(pl.multiple_of(half * half_heads, 8), half_heads)
    col_ref[...] = (row - jnp.log(dt_ref[rows, :]) * LOG2E).T
    for j in range(half_heads // 2):
        at = half * half_heads + 2 * j
        skip_rows_ref[pl.ds(j, 1), :] = jnp.where(low, skip_ref[at], skip_ref[at + 1])


def own_kernel(
    head_dim, len_ref, skip_ref, ld_ref, dt_ref, b_ref, c_ref, rowo_ref, data_in, x_ref, dy_ref,
    data_ref, x1_ref, sub1_ref, x2_ref, sub2_ref, d_ref, cb_ref,
    w_ref, rows_ref, row_ref, col_ref, skip_rows_ref, colo_ref, skipo_ref,
    task_w_ref, spread_ref, sems
):
    idx, mine, lower = place()
    kind1 = jnp.where(lower, 0, 1)
    kinds = (kind1, 1 - kind1)
    span = ld_ref.shape[1]
    half_heads = ld_ref.shape[0] // 2
    sub = span // 2
    valid = len_ref[0] - idx * span
    wait = load_tasks(((True, True), (False, True)), kinds, mine, x_ref, dy_ref, data_ref, sems)
    rows = pl.ds(pl.multiple_of(mine * half_heads, 8), half_heads)
    cum, ws, wg, d_a, d_b = weights(ld_ref[rows, :], dt_ref[rows, :])
    w_ref[0] = ws
    w_ref[1] = wg
    rows_ref[0] = spread(d_a, spread_ref, head_dim)
    rows_ref[1] = spread(d_b, spread_ref, head_dim)
    row = cum * LOG2E
    row_ref[...] = row
    d_ref[...] = rows_ref[0] * rows_ref[1]
    more_tables(mine, head_dim, row, dt_ref, skip_ref, col_ref, skip_rows_ref)
    more_tables(1 - mine, head_dim, rowo_ref[...], dt_ref, skip_ref, colo_ref, skipo_ref)
    for s in range(2):
        cols = slice(s * sub, (s + 1) * sub)
        dots = mm(b_ref[:, cols], c_ref[:, cols], TN)
        cb_ref[s] = jnp.where(iota(dots.shape, 1) >= iota(dots.shape, 0), dots, 0.0)
    b, c = b_ref[...].astype(F32), c_ref[...].astype(F32)
    for t, (total_ref, sub_ref) in enumerate(((x1_ref, sub1_ref), (x2_ref, sub2_ref))):
        task_w_ref[t] = jnp.where(kinds[t] == 0, ws, wg)
        run_task(
            t, kinds[t], OWN, valid, wait, sems.shape[1], head_dim, b, c, task_w_ref.at[t],
            rows_ref, data_ref, total_ref, sub_ref,
        )


def table_shapes(heads, span):
    shape = jax.ShapeDtypeStruct
    half, pairs = heads // 2, heads // 4
    return [
        shape((2, half, span), F32),
        shape((2, pairs, LANES), F32),
        shape((half, span), F32),
        shape((span, half), F32),
        shape((pairs, LANES), F32),
    ]


def own_part(length, skip, ld, dt, b, c, row_other, data, x, dy):
    heads, span = ld.shape
    columns = x.shape[1]
    states = b.shape[0]
    pairs = heads // 4
    sub = span // 2
    shape = jax.ShapeDtypeStruct
    tile = shape((columns // 2 // LANES, states, LANES), F32)
    outs = [shape(data.shape, BF16), tile, tile, tile, tile, shape((pairs, LANES), F32)]
    outs += [shape((2, sub, sub), F32)]
    outs += table_shapes(heads, span) + table_shapes(heads, span)[3:]
    return pl.pallas_call(
        functools.partial(own_kernel, columns // heads),
        out_shape=outs,
        in_specs=[smem(), smem()] + [whole() for _ in range(6)] + [hbm(), hbm()],
        out_specs=[whole() for _ in outs],
        scratch_shapes=[
            pltpu.VMEM((2, heads // 2, span), F32),
            pltpu.VMEM((heads // 2, LANES), F32),
            pltpu.SemaphoreType.DMA((2, 4)),
        ],
        input_output_aliases={7: 0},
        compiler_params=pltpu.CompilerParams(vmem_limit_bytes=12 << 20),
        name="own",
    )(length, skip, ld, dt, b, c, row_other, data, x, dy)


def pair_flags(second):
    idx, mine, lower = place()
    ahead = jnp.where(lower, mine == 0, mine == 1)
    return jnp.logical_not(ahead) if second else ahead


def inner_unit():
    unit = lax.axis_index("seq") // 2
    return jnp.logical_or(unit == 1, unit == 2)


def wide_rows(ref, tiles):
    both = ref[tiles:]
    both = both.reshape(both.shape[0] * both.shape[1], LANES).astype(F32)
    count = both.shape[0] // 2
    return both[:count] + both[count:]


def narrow_rows(rows):
    high = rows.astype(BF16).astype(F32)
    return jnp.concatenate([high, rows - high], axis=0).astype(BF16)


def pair_total(ahead, d, dp, x, y):
    return jnp.where(ahead, dp, d) * jnp.where(ahead, x, y) + jnp.where(ahead, y, x)


def hand_on(ahead, d, dp, x, y, carry):
    passed = jnp.where(ahead, d, dp) * carry + jnp.where(ahead, x, y)
    return jnp.where(ahead, carry, passed), jnp.where(ahead, passed, carry)


def total_kernel(second, mine_ref, x_ref, y_ref, *refs):
    out_ref, dp_ref = refs[-2:]
    ahead = pair_flags(second)
    tiles = x_ref.shape[0]
    dp_ref[...] = wide_rows(y_ref, 2 * tiles)
    base = tiles if second else 0
    if not second:
        rows = narrow_rows(dp_ref[...] * mine_ref[...])
        out_ref[tiles:] = rows.reshape((out_ref.shape[0] - tiles,) + out_ref.shape[1:])
    for j in range(tiles):
        dp, d = dp_ref[pl.ds(j, 1), :], mine_ref[pl.ds(j, 1), :]
        total = pair_total(ahead, d, dp, x_ref[j], y_ref[base + j].astype(F32))
        out_ref[j] = total.astype(BF16)


def near_kernel(mine_ref, x_ref, y_ref, r_ref, *refs):
    msg_ref, own_ref, send_ref, dp_ref, pd_ref = refs[-5:]
    ahead = pair_flags(False)
    inner = inner_unit()
    tiles = x_ref.shape[0]
    dp_ref[...] = wide_rows(y_ref, 2 * tiles)
    pd_ref[...] = wide_rows(r_ref, tiles)
    for j in range(tiles):
        dp, d, pd = dp_ref[pl.ds(j, 1), :], mine_ref[pl.ds(j, 1), :], pd_ref[pl.ds(j, 1), :]
        x, y, got = x_ref[j], y_ref[j].astype(F32), r_ref[j].astype(F32)
        total = pair_total(ahead, d, dp, x, y)
        joined = jnp.where(inner, d * dp, pd) * jnp.where(inner, got, total) + jnp.where(
            inner, total, got
        )
        msg_ref[j] = joined.astype(BF16)
        own, send = hand_on(ahead, d, dp, x, y, jnp.where(inner, got, 0.0))
        own_ref[j] = own.astype(BF16)
        send_ref[j] = send.astype(BF16)


def far_kernel(mine_ref, x_ref, y_ref, r_ref, r2_ref, far_ref, *refs):
    own_ref, send_ref, dp_ref, pd_ref = refs[-4:]
    ahead = pair_flags(True)
    inner = inner_unit()
    tiles = x_ref.shape[0]
    dp_ref[...] = wide_rows(y_ref, 2 * tiles)
    pd_ref[...] = wide_rows(r_ref, tiles)
    for j in range(tiles):
        dp, d, pd = dp_ref[pl.ds(j, 1), :], mine_ref[pl.ds(j, 1), :], pd_ref[pl.ds(j, 1), :]
        x, y = x_ref[j], y_ref[tiles + j].astype(F32)
        far = far_ref[j].astype(F32)
        carry = jnp.where(inner, far, r2_ref[j].astype(F32) + pd * far)
        own, send = hand_on(ahead, d, dp, x, y, carry)
        own_ref[j] = own.astype(BF16)
        send_ref[j] = send.astype(BF16)


def small_call(kernel, name, outs, rows_shape, scratch, args, after=()):
    return pl.pallas_call(
        kernel,
        out_shape=[jax.ShapeDtypeStruct(o, BF16) for o in outs],
        in_specs=[whole() for _ in args] + [pl.BlockSpec(memory_space=pl.ANY) for _ in after],
        out_specs=[whole() for _ in outs],
        scratch_shapes=[pltpu.VMEM(rows_shape, F32)] * scratch,
        compiler_params=pltpu.CompilerParams(vmem_limit_bytes=4 << 20),
        name=name,
    )(*args, *after)


def intra_kernel(rel, pair0, pairs, head_dim, first, row_ref, col_ref, cb_ref, skip_ref, data_ref, *refs):
    mix_in = None if first else refs[0]
    part_ref, mix_ref = refs[-2:]
    sub = cb_ref.shape[1]
    lane = iota((1, LANES), 1)
    keep = [
        (lane < head_dim).astype(F32).astype(BF16),
        (lane >= head_dim).astype(F32).astype(BF16),
    ]
    for s in range(2):
        here = pl.ds(s * sub, sub)
        acc = None if first else mix_in[s]
        for p in range(pairs):
            cols = pl.ds((pair0 + p) * LANES, LANES)
            xs = data_ref[rel, 0, here, cols]
            ys = data_ref[rel, 1, here, cols]
            split = jnp.concatenate([ys * keep[0], ys * keep[1]], axis=0)
            scores = mm(xs, split, NT)
            kernels = []
            for j in range(2):
                h = 2 * (pair0 + p) + j
                row = row_ref[pl.ds(h, 1), here]
                col = col_ref[here, pl.ds(h, 1)]
                decay = jnp.exp2(jnp.minimum(row - col, 100.0))
                kernels.append((decay * cb_ref[s]).astype(BF16))
                term = decay * scores[:, j * sub : (j + 1) * sub]
                acc = term if acc is None else acc + term
            within = mm(jnp.concatenate(kernels, axis=1), split)
            skip = skip_ref[pl.ds(pair0 + p, 1), :]
            part_ref[here, pl.ds(p * LANES, LANES)] = (
                within + skip * ys.astype(F32)
            ).astype(part_ref.dtype)
        mix_ref[s] = acc


def intra(rel, pair0, pairs, head_dim, row, col, cb, skip, data, mix, after=()):
    span = data.shape[2]
    args = [row, col, cb, skip, data] + ([] if mix is None else [mix])
    heads = 2 * pairs
    return pl.pallas_call(
        functools.partial(intra_kernel, rel, pair0, pairs, head_dim, mix is None),
        out_shape=[
            jax.ShapeDtypeStruct((span, pairs * LANES), BF16),
            jax.ShapeDtypeStruct(cb.shape, F32),
        ],
        in_specs=[whole() for _ in args] + [pl.BlockSpec(memory_space=pl.ANY) for _ in after],
        out_specs=[whole(), whole()],
        compiler_params=pltpu.CompilerParams(vmem_limit_bytes=16 << 20),
        cost_estimate=pl.CostEstimate(
            flops=heads * 2 * span * span * 128,
            transcendentals=heads * span * span // 2,
            bytes_accessed=heads * head_dim * span * 2 * 3,
        ),
        name="intra",
    )(*args, *after)


def inter_kernel(last, head_dim, slabs, scale_b, scale_c, b_ref, c_ref, w_ref, rows_ref, data_ref,
                 one_ref, two_ref, sub1_ref, sub2_ref, *refs):
    idx, mine, lower = place()
    rel = OTHER if last else OWN
    parts = refs[:slabs]
    refs = refs[slabs:]
    if last:
        gb_in, gc_in, slab_in, out_ref, gb_ref, gc_ref, buf_ref, sems = refs
    else:
        mix_ref, buf_ref, gb_ref, gc_ref = refs
    span, width = data_ref.shape[2:]
    sub = span // 2
    states = b_ref.shape[0]
    per = SLAB // head_dim
    if last:
        own_copy = pltpu.make_async_copy(
            slab_in, out_ref.at[:, pl.ds(pl.multiple_of(mine * width, LANES), width)], sems.at[0]
        )
        own_copy.start()
    rowhead = iota((per * states, SLAB), 0) // states
    lanehead = iota((per * states, SLAB), 1) // head_dim
    diag = (rowhead == lanehead).astype(F32).astype(BF16)
    b = b_ref[...].astype(F32)
    groups = width // SLAB
    slab_width = width // slabs
    gb = [None, None]
    gc = [None, None]
    copies = []
    sends = 1 if not last else sems.shape[0] - 1
    for g in range(groups):
        j = 2 * g
        pair = lambda ref: jnp.concatenate([ref[j], ref[j + 1]], axis=1)
        one, two, sub1, sub2 = pair(one_ref), pair(two_ref), pair(sub1_ref), pair(sub2_ref)
        grad = jnp.where(lower, two, one)
        state = jnp.where(lower, one, two)
        grad_sub = jnp.where(lower, sub2, sub1)
        state_sub = jnp.where(lower, sub1, sub2)
        row = lambda k: jnp.concatenate(
            [rows_ref[k, pl.ds(j, 1), :], rows_ref[k, pl.ds(j + 1, 1), :]], axis=1
        )
        grads = [(grad_sub + row(1) * grad.astype(F32)).astype(BF16), grad]
        states_in = [state, (state_sub + row(0) * state.astype(F32)).astype(BF16)]
        cols = pl.ds(g * SLAB, SLAB)
        part = parts[g * SLAB // slab_width]
        part_cols = pl.ds(g * SLAB % slab_width, SLAB)
        for s in range(2):
            here = pl.ds(s * sub, sub)
            rows_s = [w_ref[0, pl.ds(per * g + i, 1), here] for i in range(per)]
            rows_g = [w_ref[1, pl.ds(per * g + i, 1), here] for i in range(per)]
            grad_diag = jnp.concatenate([grads[s]] * per, axis=0) * diag
            state_diag = jnp.concatenate([states_in[s]] * per, axis=0) * diag
            bs = b[:, s * sub : (s + 1) * sub]
            left = jnp.concatenate([(bs * r).astype(BF16) for r in rows_s], axis=0)
            across = mm(left, grad_diag, TN)
            buf_ref[here, cols] = (part[here, part_cols].astype(F32) + across).astype(BF16)
            rb = mm(grad_diag, data_ref[rel, 0, here, cols], NT)
            rc = mm(state_diag, data_ref[rel, 1, here, cols], NT)
            for i in range(per):
                rows = slice(i * states, (i + 1) * states)
                tb, tc = rows_s[i] * rb[rows], rows_g[i] * rc[rows]
                gb[s] = tb if gb[s] is None else gb[s] + tb
                gc[s] = tc if gc[s] is None else gc[s] + tc
        if last and (g + 1) % (groups // sends) == 0:
            k = (g + 1) // (groups // sends) - 1
            wide = width // sends
            start = pl.multiple_of((1 - mine) * width + k * wide, LANES)
            send = pltpu.make_async_copy(
                buf_ref.at[:, pl.ds(k * wide, wide)],
                out_ref.at[:, pl.ds(start, wide)],
                sems.at[k + 1],
            )
            send.start()
            copies.append(send)
    gb = jnp.concatenate(gb, axis=1)
    gc = jnp.concatenate(gc, axis=1)
    if last:
        gb_ref[...] = (gb_in[...] + gb) * scale_b
        gc_ref[...] = (gc_in[...] + gc) * scale_c
        own_copy.wait()
        for send in copies:
            send.wait()
    else:
        mixed_b, mixed_c = [], []
        for s in range(2):
            here = slice(s * sub, (s + 1) * sub)
            keep = iota((sub, sub), 1) >= iota((sub, sub), 0)
            mix = jnp.where(keep, mix_ref[s], 0.0)
            high = mix.astype(BF16)
            rest = (mix - high.astype(F32)).astype(BF16)
            bs, cs = b_ref[:, here], c_ref[:, here]
            mixed_b.append(mm(cs, high, NT) + mm(cs, rest, NT))
            mixed_c.append(mm(bs, high) + mm(bs, rest))
        gb_ref[...] = gb + jnp.concatenate(mixed_b, axis=1)
        gc_ref[...] = gc + jnp.concatenate(mixed_c, axis=1)


def inter(last, head_dim, scale_b, scale_c, b, c, w, rows, data, one, two, sub1, sub2, parts, extra):
    states = b.shape[0]
    span, width = data.shape[2:]
    small = jax.ShapeDtypeStruct((states, span), F32)
    args = [b, c, w, rows, data, one, two, sub1, sub2, *parts, *extra]
    sends = 4
    if last:
        out0, spec0 = jax.ShapeDtypeStruct((span, 2 * width), BF16), hbm()
        scratch = [pltpu.VMEM((span, width), BF16), pltpu.SemaphoreType.DMA((sends + 1,))]
    else:
        out0, spec0 = jax.ShapeDtypeStruct((span, width), BF16), whole()
        scratch = []
    return pl.pallas_call(
        functools.partial(inter_kernel, last, head_dim, len(parts), scale_b, scale_c),
        out_shape=[out0, small, small],
        in_specs=[whole() for _ in args],
        out_specs=[spec0, whole(), whole()],
        scratch_shapes=scratch,
        compiler_params=pltpu.CompilerParams(vmem_limit_bytes=16 << 20),
        cost_estimate=pl.CostEstimate(
            flops=width * 2 * span * 256 * 3,
            transcendentals=0,
            bytes_accessed=width * span * 2 * 4,
        ),
        name="inter",
    )(*args)


def local(inputs, out_grad, step_size, log_decay, b_matrix, c_matrix, skip_gain, lengths):
    x, dy = inputs[0], out_grad[0]
    tokens, columns = x.shape
    heads = step_size.shape[1]
    states = b_matrix.shape[1]
    head_dim = columns // heads
    count = lax.axis_size("seq")
    units = count // 2
    if tokens != SPAN or count % 4:
        raise ValueError("unsupported sizes")
    scale_b = 1.0 / math.sqrt(columns)
    scale_c = math.sqrt(states / (columns * count * tokens))
    def swap(v, bit):
        return lax.ppermute(v, "seq", [(i, i ^ bit) for i in range(count)])

    fixed = lambda v: pltpu.with_memory_space_constraint(v, pltpu.HBM)
    x, dy = fixed(x), fixed(dy)
    small = [fixed(v) for v in (log_decay[0], step_size[0], b_matrix[0], c_matrix[0])]
    msg, sub1_other, sub2_other, data, ld, dt, b, c, *other = first_part(lengths, *small, x, dy)
    y = swap(msg, 1)
    data, x1, sub1, x2, sub2, d, cb, *tables = own_part(
        lengths, skip_gain, ld, dt, b, c, other[2], data, x, dy
    )
    own, other = tables[:5], other + tables[5:]
    calls = 3
    pairs = heads // 4 // calls
    parts = {OTHER: [], OWN: []}

    def block(rel, k, mix, after=()):
        table = own if rel == OWN else other
        part, mix = intra(
            rel, k * pairs, pairs, head_dim, table[2], table[3], cb, table[4], data, mix, after
        )
        parts[rel].append(part)
        return mix

    mix = block(OWN, 0, None)
    tile = x1.shape
    if units == 4:
        (m1,) = small_call(
            functools.partial(total_kernel, False), "total", [(msg.shape[0] - tile[0],) + tile[1:]], d.shape, 1,
            [d, x1, y], [mix],
        )
        r1 = swap(m1, 2)
        (m2,) = small_call(
            functools.partial(total_kernel, True), "total", [tile], d.shape, 1, [d, x2, y], [m1]
        )
        r2 = swap(m2, 2)
        mix = block(OWN, 1, mix, [m2])
        far, own1, send1 = small_call(near_kernel, "near", [tile] * 3, d.shape, 2, [d, x1, y, r1], [mix])
        r3 = swap(far, 4)
        got1 = swap(send1, 1)
        mix = block(OWN, 2, mix, [far])
        mix = block(OTHER, 0, mix)
        mix = block(OTHER, 1, mix)
        own2, send2 = small_call(
            far_kernel, "far", [tile] * 2, d.shape, 2, [d, x2, y, r1, r2, r3], [mix]
        )
        got2 = swap(send2, 1)
    else:
        mix = block(OWN, 1, mix)
        mix = block(OWN, 2, mix)
        mix = block(OTHER, 0, mix)
        mix = block(OTHER, 1, mix)
        (own1, send1), (own2, send2) = gathered(units, d, x1, x2, y)
        got1, got2 = swap(send1, 1), swap(send2, 1)
    mix = block(OTHER, 2, mix, [send2])
    w, rows = own[:2]
    slab, gb, gc = inter(
        False, head_dim, scale_b, scale_c, b, c, w, rows, data, own1, own2, sub1, sub2,
        parts[OWN], [mix],
    )
    out, gb, gc = inter(
        True, head_dim, scale_b, scale_c, b, c, other[0], other[1], data, got1, got2,
        sub1_other, sub2_other, parts[OTHER], [gb, gc, slab],
    )
    return (out[None], gb[None], gc[None])


def gathered(units, d, x1, x2, y):
    idx = lax.axis_index("seq")
    mine, unit = idx % 2, idx // 2
    lower = unit < units // 2
    tiles = x1.shape[0]
    dp = wide_rows(y, 2 * tiles)[:, None, :]
    d = d[:, None, :]
    ys = (y[:tiles].astype(F32), y[tiles : 2 * tiles].astype(F32))
    xs = (x1, x2)
    totals = [pair_total(pair_flags(k == 1), d, dp, xs[k], ys[k]) for k in range(2)]
    own_half = lambda v: jnp.take(lax.all_gather(v, "seq"), 2 * jnp.arange(units) + mine, axis=0)
    forward = own_half(jnp.where(lower, totals[0], totals[1]))
    backward = own_half(jnp.where(lower, totals[1], totals[0]))
    decays = own_half(d * dp)
    state = grad = jnp.zeros_like(x1)
    for u in range(units):
        state = jnp.where(u < unit, decays[u] * state + forward[u], state)
        v = units - 1 - u
        grad = jnp.where(v > unit, decays[v] * grad + backward[v], grad)
    carries = (jnp.where(lower, state, grad), jnp.where(lower, grad, state))
    outs = [hand_on(pair_flags(k == 1), d, dp, xs[k], ys[k], carries[k]) for k in range(2)]
    return [[v.astype(BF16) for v in pair] for pair in outs]


def solution(mesh):
    placed = (
        P("batch", "seq", None),
        P("batch", "seq", None),
        P("batch", None, "seq"),
        P("batch", None, "seq"),
        P("batch", None, "seq"),
        P("batch", None, "seq"),
        P(),
        P("batch"),
    )
    return jax.shard_map(
        local,
        mesh=mesh,
        in_specs=placed,
        out_specs=(P("batch", "seq", None), P("batch", None, "seq"), P("batch", None, "seq")),
        check_vma=False,
    )
```

```python
import functools
import math

import jax
import jax.numpy as jnp
from jax import lax
from jax.experimental import pallas as pl
from jax.experimental.pallas import tpu as pltpu
from jax.sharding import PartitionSpec as P

SPAN = 256
LANES = 128
SLAB = 2 * LANES
LOG2E = math.log2(math.e)
F32 = jnp.float32
BF16 = jnp.bfloat16
NT = (((1,), (1,)), ((), ()))
TN = (((0,), (0,)), ((), ()))
OTHER, OWN = 0, 1


def place():
    idx = lax.axis_index("seq")
    count = lax.axis_size("seq")
    return idx, lax.rem(idx, 2), idx < count // 2


def mm(a, b, dims=None):
    if dims is None:
        return jnp.dot(a, b, preferred_element_type=F32)
    return lax.dot_general(a, b, dims, preferred_element_type=F32)


def pick(condition, a, b):
    if isinstance(condition, bool):
        return a if condition else b
    return jnp.where(condition, a, b)


def whole():
    return pl.BlockSpec(memory_space=pltpu.VMEM)


def smem():
    return pl.BlockSpec(memory_space=pltpu.SMEM)


def hbm():
    return pl.BlockSpec(memory_space=pltpu.HBM)


def iota(shape, axis):
    return lax.broadcasted_iota(jnp.int32, shape, axis)


def running_sum(values):
    rows, span = values.shape
    sub = span // 2
    high = values.astype(BF16)
    rest = values - high.astype(F32)
    middle = rest.astype(BF16)
    low = (rest - middle.astype(F32)).astype(BF16)
    upper = (iota((sub, sub), 0) <= iota((sub, sub), 1)).astype(F32).astype(BF16)
    pieces = jnp.concatenate([high, middle, low], axis=0)
    halves = []
    for s in range(2):
        sums = mm(pieces[:, s * sub : (s + 1) * sub], upper)
        halves.append(sums[:rows] + sums[rows : 2 * rows] + sums[2 * rows :])
    return jnp.concatenate(halves, axis=1)


def weights(ld, dt, valid):
    cum = running_sum(ld)
    rows, span = cum.shape
    sub = span // 2
    end_a, end_b = cum[:, sub - 1 : sub], cum[:, span - 1 : span]
    ends = jnp.where(iota(cum.shape, 1) < sub, end_a, end_b)
    into_grad = jnp.where(iota(cum.shape, 1) < valid, jnp.exp(cum), 0.0)
    return cum, dt * jnp.exp(ends - cum), into_grad, jnp.exp(end_a), jnp.exp(end_b)


def spread(column, scratch_ref, head_dim):
    rows = scratch_ref.shape[0]
    scratch_ref[...] = jnp.broadcast_to(column, scratch_ref.shape)
    even = scratch_ref[pl.ds(0, rows // 2, stride=2), :]
    odd = scratch_ref[pl.ds(1, rows // 2, stride=2), :]
    return jnp.where(iota(even.shape, 1) < head_dim, even, odd)


def run_task(is_state, weight, read, chunks, head_dim, mat, w_ref, rows_ref, put, span, width):
    sub = span // 2
    states = mat.shape[0]
    per = SLAB // head_dim
    low = iota((states, LANES), 1) < head_dim
    w_ref[...] = weight
    chunk = width // chunks
    for g in range(width // SLAB):
        if g * SLAB % chunk == 0:
            read(None, g * SLAB // chunk)
        lhs = jnp.concatenate(
            [(mat * w_ref[pl.ds(per * g + j, 1), :]).astype(BF16) for j in range(per)], axis=0
        )
        parts = [mm(lhs[:, s * sub : (s + 1) * sub], read(s, g)) for s in range(2)]
        for q in range(2):
            lanes = slice(q * LANES, (q + 1) * LANES)
            top = slice(2 * q * states, (2 * q + 1) * states)
            bottom = slice((2 * q + 1) * states, (2 * q + 2) * states)
            e0, e1 = [jnp.where(low, p[top, lanes], p[bottom, lanes]) for p in parts]
            j = 2 * g + q
            d_a, d_b = rows_ref[0, pl.ds(j, 1), :], rows_ref[1, pl.ds(j, 1), :]
            if isinstance(is_state, bool):
                total = d_b * e0 + e1 if is_state else e0 + d_a * e1
            else:
                total = jnp.where(is_state, d_b, 1.0) * e0 + jnp.where(is_state, 1.0, d_a) * e1
            put(j, total, pick(is_state, e0, e1))


def first_kernel(
    head_dim, len_ref, ld_hbm, dt_hbm, b_hbm, c_hbm, x_ref, dy_ref,
    msg_ref, sub_ref, ld_ref, dt_ref, b_ref, c_ref, w_ref, rows_ref, row_ref,
    data_ref, task_w_ref, spread_ref, sems, small_sems
):
    idx, mine, lower = place()
    span = ld_ref.shape[1]
    sub = span // 2
    half_heads = ld_ref.shape[0] // 2
    width = data_ref.shape[1]
    chunks = sems.shape[0]
    chunk = width // chunks
    small = [
        pltpu.make_async_copy(src, dst, small_sems.at[i])
        for i, (src, dst) in enumerate(
            ((ld_hbm, ld_ref), (dt_hbm, dt_ref), (b_hbm, b_ref), (c_hbm, c_ref))
        )
    ]
    for copy in small:
        copy.start()

    def fetch(i, src):
        start = pl.multiple_of((1 - mine) * width + i * chunk, LANES)
        return pltpu.make_async_copy(
            src.at[:, pl.ds(start, chunk)], data_ref.at[:, pl.ds(i * chunk, chunk)], sems.at[i]
        )

    for i in range(chunks):

        @pl.when(lower)
        def _():
            fetch(i, x_ref).start()

        @pl.when(jnp.logical_not(lower))
        def _():
            fetch(i, dy_ref).start()

    for copy in small:
        copy.wait()
    rows = pl.ds(pl.multiple_of((1 - mine) * half_heads, 8), half_heads)
    valid = len_ref[0] - idx * span
    cum, ws, wg, d_a, d_b = weights(ld_ref[rows, :], dt_ref[rows, :], valid)
    w_ref[0] = ws
    w_ref[1] = wg
    row_ref[...] = cum * LOG2E
    rows_a = spread(d_a, spread_ref, head_dim)
    rows_b = spread(d_b, spread_ref, head_dim)
    rows_ref[0] = rows_a
    rows_ref[1] = rows_b
    tiles = sub_ref.shape[0]
    extra = narrow_rows(rows_a * rows_b)
    msg_ref[tiles:] = extra.reshape((msg_ref.shape[0] - tiles,) + msg_ref.shape[1:])

    def read(s, g):
        if s is None:
            return fetch(g, x_ref).wait()
        return data_ref[pl.ds(s * sub, sub), pl.ds(g * SLAB, SLAB)]

    def put(j, total, part):
        msg_ref[j] = total.astype(BF16)
        sub_ref[j] = part

    mat = jnp.where(lower, b_ref[...].astype(F32), c_ref[...].astype(F32))
    run_task(
        lower, jnp.where(lower, ws, wg), read, chunks, head_dim, mat, task_w_ref, rows_ref, put, span, width
    )


def first_part(length, ld, dt, b, c, x, dy):
    heads, span = ld.shape
    columns = x.shape[1]
    states = b.shape[0]
    tiles = columns // 2 // LANES
    pairs = heads // 4
    shape = jax.ShapeDtypeStruct
    tile = lambda n, t: shape((n, states, LANES), t)
    same = lambda a: shape(a.shape, a.dtype)
    outs = [
        tile(tiles + 2 * pairs // states, BF16),
        tile(tiles, F32),
        same(ld), same(dt), same(b), same(c),
    ] + table_shapes(heads, span)[:3]
    return pl.pallas_call(
        functools.partial(first_kernel, columns // heads),
        out_shape=outs,
        in_specs=[smem()] + [hbm() for _ in range(6)],
        out_specs=[whole() for _ in outs],
        scratch_shapes=[
            pltpu.VMEM((span, columns // 2), BF16),
            pltpu.VMEM((heads // 2, span), F32),
            pltpu.VMEM((heads // 2, LANES), F32),
            pltpu.SemaphoreType.DMA((4,)),
            pltpu.SemaphoreType.DMA((4,)),
        ],
        compiler_params=pltpu.CompilerParams(vmem_limit_bytes=8 << 20),
        name="first",
    )(length, ld, dt, b, c, x, dy)


def more_tables(half, head_dim, row, dt_ref, skip_ref, col_ref, skip_rows_ref):
    half_heads = row.shape[0]
    low = iota((1, LANES), 1) < head_dim
    rows = pl.ds(pl.multiple_of(half * half_heads, 8), half_heads)
    col_ref[...] = (row - jnp.log(dt_ref[rows, :]) * LOG2E).T
    for j in range(half_heads // 2):
        at = half * half_heads + 2 * j
        skip_rows_ref[pl.ds(j, 1), :] = jnp.where(low, skip_ref[at], skip_ref[at + 1])


def own_kernel(
    head_dim, len_ref, skip_ref, ld_ref, dt_ref, b_ref, c_ref, wo_ref, rowso_ref, rowo_ref, x_ref, dy_ref,
    xs_ref, subs_ref, send_ref, subo_ref, d_ref, cb_ref,
    w_ref, rows_ref, row_ref, col_ref, skip_rows_ref, colo_ref, skipo_ref,
    task_w_ref, spread_ref
):
    idx, mine, lower = place()
    span = ld_ref.shape[1]
    half_heads = ld_ref.shape[0] // 2
    width = x_ref.shape[1] // 2
    sub = span // 2
    valid = len_ref[0] - idx * span
    rows = pl.ds(pl.multiple_of(mine * half_heads, 8), half_heads)
    cum, ws, wg, d_a, d_b = weights(ld_ref[rows, :], dt_ref[rows, :], valid)
    w_ref[0] = ws
    w_ref[1] = wg
    rows_ref[0] = spread(d_a, spread_ref, head_dim)
    rows_ref[1] = spread(d_b, spread_ref, head_dim)
    row = cum * LOG2E
    row_ref[...] = row
    d_ref[...] = rows_ref[0] * rows_ref[1]
    more_tables(mine, head_dim, row, dt_ref, skip_ref, col_ref, skip_rows_ref)
    more_tables(1 - mine, head_dim, rowo_ref[...], dt_ref, skip_ref, colo_ref, skipo_ref)
    for s in range(2):
        cols = slice(s * sub, (s + 1) * sub)
        dots = mm(b_ref[:, cols], c_ref[:, cols], TN)
        t, u = iota(dots.shape, 0), iota(dots.shape, 1)
        cb_ref[s] = jnp.where(jnp.logical_and(u >= t, u + s * sub < valid), dots, 0.0)
    b, c = b_ref[...].astype(F32), c_ref[...].astype(F32)
    kind_slot = jnp.where(lower, 0, 1)

    def reader(ref, half):
        def read(s, g):
            if s is None:
                return None
            start = pl.multiple_of(half * width + g * SLAB, LANES)
            return ref[pl.ds(s * sub, sub), pl.ds(start, SLAB)]

        return read

    def putter(slot):
        def put(j, total, part):
            xs_ref[slot, j] = total
            subs_ref[slot, j] = part

        return put

    def put_other(j, total, part):
        send_ref[j] = total.astype(BF16)
        subo_ref[j] = part

    run_task(
        True, ws, reader(x_ref, mine), 1, head_dim, b, task_w_ref.at[0], rows_ref, putter(kind_slot), span, width
    )
    run_task(
        False, wg, reader(dy_ref, mine), 1, head_dim, c, task_w_ref.at[1], rows_ref,
        putter(1 - kind_slot), span, width,
    )
    upper = jnp.logical_not(lower)
    read_x, read_dy = reader(x_ref, 1 - mine), reader(dy_ref, 1 - mine)

    def read_either(s, g):
        return None if s is None else jnp.where(upper, read_x(s, g), read_dy(s, g))

    run_task(
        upper, jnp.where(upper, wo_ref[0], wo_ref[1]), read_either, 1, head_dim, jnp.where(upper, b, c),
        task_w_ref.at[2], rowso_ref, put_other, span, width,
    )


def table_shapes(heads, span):
    shape = jax.ShapeDtypeStruct
    half, pairs = heads // 2, heads // 4
    return [
        shape((2, half, span), F32),
        shape((2, pairs, LANES), F32),
        shape((half, span), F32),
        shape((span, half), F32),
        shape((pairs, LANES), F32),
    ]


def own_part(length, skip, ld, dt, b, c, other, x, dy):
    heads, span = ld.shape
    columns = x.shape[1]
    states = b.shape[0]
    pairs = heads // 4
    sub = span // 2
    tiles = columns // 2 // LANES
    shape = jax.ShapeDtypeStruct
    outs = [shape((2, tiles, states, LANES), F32)] * 2
    outs += [shape((tiles, states, LANES), BF16), shape((tiles, states, LANES), F32)]
    outs += [shape((pairs, LANES), F32), shape((2, sub, sub), F32)]
    outs += table_shapes(heads, span) + table_shapes(heads, span)[3:]
    return pl.pallas_call(
        functools.partial(own_kernel, columns // heads),
        out_shape=outs,
        in_specs=[smem(), smem()] + [whole() for _ in range(9)],
        out_specs=[whole() for _ in outs],
        scratch_shapes=[
            pltpu.VMEM((3, heads // 2, span), F32),
            pltpu.VMEM((heads // 2, LANES), F32),
        ],
        compiler_params=pltpu.CompilerParams(vmem_limit_bytes=8 << 20),
        name="own",
    )(length, skip, ld, dt, b, c, *other, x, dy)


def pair_flags(second):
    idx, mine, lower = place()
    ahead = jnp.where(lower, mine == 0, mine == 1)
    return jnp.logical_not(ahead) if second else ahead


def inner_unit():
    unit = lax.axis_index("seq") // 2
    return jnp.logical_or(unit == 1, unit == 2)


def wide_rows(ref, tiles):
    both = ref[tiles:]
    both = both.reshape(both.shape[0] * both.shape[1], LANES).astype(F32)
    count = both.shape[0] // 2
    return both[:count] + both[count:]


def narrow_rows(rows):
    high = rows.astype(BF16).astype(F32)
    return jnp.concatenate([high, rows - high], axis=0).astype(BF16)


def pair_total(ahead, d, dp, x, y):
    return jnp.where(ahead, dp, d) * jnp.where(ahead, x, y) + jnp.where(ahead, y, x)


def hand_on(ahead, d, dp, x, y, carry):
    passed = jnp.where(ahead, d, dp) * carry + jnp.where(ahead, x, y)
    return jnp.where(ahead, carry, passed), jnp.where(ahead, passed, carry)


def total_kernel(second, decay_ref, mine_ref, x_ref, y_ref, *refs):
    out_ref, dp_ref = refs[-2:]
    ahead = pair_flags(second)
    tiles = x_ref.shape[1]
    dp_ref[...] = wide_rows(decay_ref, tiles)
    if not second:
        rows = narrow_rows(dp_ref[...] * mine_ref[...])
        out_ref[tiles:] = rows.reshape((out_ref.shape[0] - tiles,) + out_ref.shape[1:])
    for j in range(tiles):
        dp, d = dp_ref[pl.ds(j, 1), :], mine_ref[pl.ds(j, 1), :]
        total = pair_total(ahead, d, dp, x_ref[int(second), j], y_ref[j].astype(F32))
        out_ref[j] = total.astype(BF16)


def near_kernel(decay_ref, mine_ref, x_ref, y_ref, r_ref, *refs):
    msg_ref, own_ref, send_ref, dp_ref, pd_ref = refs[-5:]
    ahead = pair_flags(False)
    inner = inner_unit()
    tiles = x_ref.shape[1]
    dp_ref[...] = wide_rows(decay_ref, tiles)
    pd_ref[...] = wide_rows(r_ref, tiles)
    for j in range(tiles):
        dp, d, pd = dp_ref[pl.ds(j, 1), :], mine_ref[pl.ds(j, 1), :], pd_ref[pl.ds(j, 1), :]
        x, y, got = x_ref[0, j], y_ref[j].astype(F32), r_ref[j].astype(F32)
        total = pair_total(ahead, d, dp, x, y)
        joined = jnp.where(inner, d * dp, pd) * jnp.where(inner, got, total) + jnp.where(
            inner, total, got
        )
        msg_ref[j] = joined.astype(BF16)
        own, send = hand_on(ahead, d, dp, x, y, jnp.where(inner, got, 0.0))
        own_ref[j] = own.astype(BF16)
        send_ref[j] = send.astype(BF16)


def far_kernel(decay_ref, mine_ref, x_ref, y_ref, r_ref, r2_ref, far_ref, *refs):
    own_ref, send_ref, dp_ref, pd_ref = refs[-4:]
    ahead = pair_flags(True)
    inner = inner_unit()
    tiles = x_ref.shape[1]
    dp_ref[...] = wide_rows(decay_ref, tiles)
    pd_ref[...] = wide_rows(r_ref, tiles)
    for j in range(tiles):
        dp, d, pd = dp_ref[pl.ds(j, 1), :], mine_ref[pl.ds(j, 1), :], pd_ref[pl.ds(j, 1), :]
        x, y = x_ref[1, j], y_ref[j].astype(F32)
        far = far_ref[j].astype(F32)
        carry = jnp.where(inner, far, r2_ref[j].astype(F32) + pd * far)
        own, send = hand_on(ahead, d, dp, x, y, carry)
        own_ref[j] = own.astype(BF16)
        send_ref[j] = send.astype(BF16)


def small_call(kernel, name, outs, rows_shape, scratch, args, after=()):
    return pl.pallas_call(
        kernel,
        out_shape=[jax.ShapeDtypeStruct(o, BF16) for o in outs],
        in_specs=[whole() for _ in args] + [pl.BlockSpec(memory_space=pl.ANY) for _ in after],
        out_specs=[whole() for _ in outs],
        scratch_shapes=[pltpu.VMEM(rows_shape, F32)] * scratch,
        compiler_params=pltpu.CompilerParams(vmem_limit_bytes=4 << 20),
        name=name,
    )(*args, *after)


def intra_kernel(rel, pair0, pairs, head_dim, first, len_ref, row_ref, col_ref, cb_ref, skip_ref, x_ref, dy_ref, *refs):
    mix_in = None if first else refs[0]
    part_ref, mix_ref = refs[-2:]
    sub = cb_ref.shape[1]
    idx, mine, lower = place()
    base = (mine if rel == OWN else 1 - mine) * (x_ref.shape[1] // 2)
    valid = len_ref[0] - idx * x_ref.shape[0]
    lane = iota((1, LANES), 1)
    keep = [
        (lane < head_dim).astype(F32).astype(BF16),
        (lane >= head_dim).astype(F32).astype(BF16),
    ]
    for s in range(2):
        here = pl.ds(s * sub, sub)
        acc = None if first else mix_in[s]
        inside = iota((sub, LANES), 0) + s * sub < valid
        for p in range(pairs):
            cols = pl.ds(pl.multiple_of(base + (pair0 + p) * LANES, LANES), LANES)
            xs = x_ref[here, cols]
            ys = dy_ref[here, cols]
            split = jnp.concatenate([ys * keep[0], ys * keep[1]], axis=0)
            scores = mm(xs, split, NT)
            kernels = []
            for j in range(2):
                h = 2 * (pair0 + p) + j
                row = row_ref[pl.ds(h, 1), here]
                col = col_ref[here, pl.ds(h, 1)]
                decay = jnp.exp2(jnp.minimum(row - col, 100.0))
                kernels.append((decay * cb_ref[s]).astype(BF16))
                term = decay * scores[:, j * sub : (j + 1) * sub]
                acc = term if acc is None else acc + term
            within = mm(jnp.concatenate(kernels, axis=1), split)
            skip = skip_ref[pl.ds(pair0 + p, 1), :]
            part_ref[here, pl.ds(p * LANES, LANES)] = (
                within + jnp.where(inside, skip * ys.astype(F32), 0.0)
            ).astype(part_ref.dtype)
        mix_ref[s] = acc


def intra(rel, pair0, pairs, head_dim, length, row, col, cb, skip, x, dy, mix, after=()):
    span = x.shape[0]
    args = [row, col, cb, skip, x, dy] + ([] if mix is None else [mix])
    heads = 2 * pairs
    return pl.pallas_call(
        functools.partial(intra_kernel, rel, pair0, pairs, head_dim, mix is None),
        out_shape=[
            jax.ShapeDtypeStruct((span, pairs * LANES), BF16),
            jax.ShapeDtypeStruct(cb.shape, F32),
        ],
        in_specs=[smem()] + [whole() for _ in args] + [pl.BlockSpec(memory_space=pl.ANY) for _ in after],
        out_specs=[whole(), whole()],
        compiler_params=pltpu.CompilerParams(vmem_limit_bytes=8 << 20),
        cost_estimate=pl.CostEstimate(
            flops=heads * 2 * span * span * 128,
            transcendentals=heads * span * span // 2,
            bytes_accessed=heads * head_dim * span * 2 * 3,
        ),
        name="intra",
    )(length, *args, *after)


def pair_tiles(ref, g):
    return jnp.concatenate([ref[2 * g], ref[2 * g + 1]], axis=1)


def pair_rows(rows_ref, k, g):
    return jnp.concatenate(
        [rows_ref[k, pl.ds(2 * g, 1), :], rows_ref[k, pl.ds(2 * g + 1, 1), :]], axis=1
    )


def carry_pass(is_grad, carry_ref, sub_ref, data_ref, b_ref, w_ref, rows_ref, parts, buf_ref, base, head_dim, done):
    span, width = data_ref.shape[0], data_ref.shape[1] // 2
    sub = span // 2
    states = b_ref.shape[0]
    per = SLAB // head_dim
    rowhead = iota((per * states, SLAB), 0) // states
    lanehead = iota((per * states, SLAB), 1) // head_dim
    diag = (rowhead == lanehead).astype(F32).astype(BF16)
    b = b_ref[...].astype(F32) if is_grad else None
    slab_width = parts[0].shape[1] if is_grad else width
    total = [None, None]
    for g in range(width // SLAB):
        carry = pair_tiles(carry_ref, g)
        moved = pair_tiles(sub_ref, g) + pair_rows(rows_ref, int(is_grad), g) * carry.astype(F32)
        carries = [moved.astype(BF16), carry] if is_grad else [carry, moved.astype(BF16)]
        data_cols = pl.ds(pl.multiple_of(base + g * SLAB, LANES), SLAB)
        for s in range(2):
            here = pl.ds(s * sub, sub)
            rows = [w_ref[1 - int(is_grad), pl.ds(per * g + i, 1), here] for i in range(per)]
            spread_out = jnp.concatenate([carries[s]] * per, axis=0) * diag
            if is_grad:
                bs = b[:, s * sub : (s + 1) * sub]
                left = jnp.concatenate([(bs * r).astype(BF16) for r in rows], axis=0)
                across = mm(left, spread_out, TN)
                part = parts[g * SLAB // slab_width][here, pl.ds(g * SLAB % slab_width, SLAB)]
                buf_ref[here, pl.ds(g * SLAB, SLAB)] = (part.astype(F32) + across).astype(BF16)
            terms = mm(spread_out, data_ref[here, data_cols], NT)
            for i in range(per):
                term = rows[i] * terms[i * states : (i + 1) * states]
                total[s] = term if total[s] is None else total[s] + term
        done(g)
    return jnp.concatenate(total, axis=1)


class Sender:
    def __init__(self, buf_ref, out_ref, sems, base, every):
        self.buf_ref, self.out_ref, self.sems = buf_ref, out_ref, sems
        self.base, self.every, self.copies = base, every, []

    def __call__(self, g):
        if (g + 1) % self.every == 0:
            wide = self.every * SLAB
            k = len(self.copies)
            copy = pltpu.make_async_copy(
                self.buf_ref.at[:, pl.ds(k * wide, wide)],
                self.out_ref.at[:, pl.ds(pl.multiple_of(self.base + k * wide, LANES), wide)],
                self.sems.at[k],
            )
            copy.start()
            self.copies.append(copy)

    def wait(self):
        for copy in self.copies:
            copy.wait()


def inter_own_kernel(
    head_dim, slabs, len_ref, b_ref, c_ref, w_ref, rows_ref, x_ref, dy_ref, one_ref, two_ref,
    subs_ref, mix_ref, *refs
):
    idx, mine, lower = place()
    parts = refs[:slabs]
    buf_ref, gb_ref, gc_ref, pick_ref = refs[slabs:]
    span, width = x_ref.shape[0], x_ref.shape[1] // 2
    sub = span // 2
    base = mine * width
    valid = len_ref[0] - idx * span
    for j in range(one_ref.shape[0]):
        pick_ref[0, j] = jnp.where(lower, two_ref[j], one_ref[j])
        pick_ref[1, j] = jnp.where(lower, one_ref[j], two_ref[j])
    slot = jnp.where(lower, 0, 1)
    gb = carry_pass(
        True, pick_ref.at[0], subs_ref.at[1 - slot], x_ref, b_ref, w_ref, rows_ref, parts, buf_ref, base,
        head_dim, lambda g: None,
    )
    gc = carry_pass(
        False, pick_ref.at[1], subs_ref.at[slot], dy_ref, b_ref, w_ref, rows_ref, None, None, base,
        head_dim, lambda g: None,
    )
    mixed_b, mixed_c = [], []
    for s in range(2):
        here = slice(s * sub, (s + 1) * sub)
        t, u = iota((sub, sub), 0), iota((sub, sub), 1)
        mix = jnp.where(jnp.logical_and(u >= t, u + s * sub < valid), mix_ref[s], 0.0)
        high = mix.astype(BF16)
        rest = (mix - high.astype(F32)).astype(BF16)
        bs, cs = b_ref[:, here], c_ref[:, here]
        mixed_b.append(mm(cs, high, NT) + mm(cs, rest, NT))
        mixed_c.append(mm(bs, high) + mm(bs, rest))
    gb_ref[...] = gb + jnp.concatenate(mixed_b, axis=1)
    gc_ref[...] = gc + jnp.concatenate(mixed_c, axis=1)


def near_other_kernel(
    head_dim, slabs, b_ref, w_ref, rows_ref, x_ref, dy_ref, carry_ref, sub_ref, gb_in, gc_in, slab_ref, *refs
):
    idx, mine, lower = place()
    parts = refs[:slabs]
    out_ref, buf_ref, gb_ref, gc_ref, sem = refs[slabs:]
    width = x_ref.shape[1] // 2
    base = (1 - mine) * width
    start = pl.multiple_of(mine * width, LANES)
    own_copy = pltpu.make_async_copy(slab_ref, out_ref.at[:, pl.ds(start, width)], sem)
    own_copy.start()
    gb_ref[...] = gb_in[...]
    gc_ref[...] = gc_in[...]

    @pl.when(jnp.logical_not(lower))
    def _():
        gb_ref[...] += carry_pass(
            True, carry_ref, sub_ref, x_ref, b_ref, w_ref, rows_ref, parts, buf_ref, base, head_dim,
            lambda g: None,
        )

    @pl.when(lower)
    def _():
        gc_ref[...] += carry_pass(
            False, carry_ref, sub_ref, dy_ref, b_ref, w_ref, rows_ref, None, None, base, head_dim,
            lambda g: None,
        )

    own_copy.wait()


def far_other_kernel(
    head_dim, slabs, every, scale_b, scale_c, b_ref, w_ref, rows_ref, x_ref, dy_ref, carry_ref, sub_ref,
    gb_in, gc_in, slab_ref, out_in, *refs
):
    idx, mine, lower = place()
    parts = refs[:slabs]
    out_ref, gb_out, gc_out, buf_ref, gb_ref, gc_ref, sems, small_sems = refs[slabs:]
    width = x_ref.shape[1] // 2
    base = (1 - mine) * width
    gb_ref[...] = gb_in[...] * scale_b
    gc_ref[...] = gc_in[...] * scale_c
    copies = [
        pltpu.make_async_copy(src, dst, small_sems.at[i])
        for i, (src, dst) in enumerate(((gb_ref, gb_out), (gc_ref, gc_out)))
    ]

    @pl.when(lower)
    def _():
        send = Sender(buf_ref, out_ref, sems, base, every)
        gb_ref[...] += scale_b * carry_pass(
            True, carry_ref, sub_ref, x_ref, b_ref, w_ref, rows_ref, parts, buf_ref, base, head_dim, send
        )
        for copy in copies:
            copy.start()
        send.wait()

    @pl.when(jnp.logical_not(lower))
    def _():
        start = pl.multiple_of(base, LANES)
        slab_copy = pltpu.make_async_copy(slab_ref, out_ref.at[:, pl.ds(start, width)], small_sems.at[2])
        slab_copy.start()
        gc_ref[...] += scale_c * carry_pass(
            False, carry_ref, sub_ref, dy_ref, b_ref, w_ref, rows_ref, None, None, base, head_dim,
            lambda g: None,
        )
        for copy in copies:
            copy.start()
        slab_copy.wait()

    for copy in copies:
        copy.wait()


def inter_cost(width, span, passes):
    return pl.CostEstimate(
        flops=width * 2 * span * 256 * passes, transcendentals=0, bytes_accessed=width * span * 2 * 4
    )


def inter_own(head_dim, length, b, c, w, rows, x, dy, one, two, subs, mix, parts):
    states = b.shape[0]
    span, width = x.shape[0], x.shape[1] // 2
    small = jax.ShapeDtypeStruct((states, span), F32)
    args = [b, c, w, rows, x, dy, one, two, subs, mix, *parts]
    return pl.pallas_call(
        functools.partial(inter_own_kernel, head_dim, len(parts)),
        out_shape=[jax.ShapeDtypeStruct((span, width), BF16), small, small],
        in_specs=[smem()] + [whole() for _ in args],
        out_specs=[whole(), whole(), whole()],
        scratch_shapes=[pltpu.VMEM((2,) + one.shape, BF16)],
        compiler_params=pltpu.CompilerParams(vmem_limit_bytes=12 << 20),
        cost_estimate=inter_cost(width, span, 3),
        name="inter_own",
    )(length, *args)


def near_other(head_dim, b, w, rows, x, dy, carry, sub, gb, gc, slab, parts):
    span, width = slab.shape
    args = [b, w, rows, x, dy, carry, sub, gb, gc, slab, *parts]
    return pl.pallas_call(
        functools.partial(near_other_kernel, head_dim, len(parts)),
        out_shape=[
            jax.ShapeDtypeStruct(v, t)
            for v, t in (((span, 2 * width), BF16), (slab.shape, BF16), (gb.shape, F32), (gc.shape, F32))
        ],
        in_specs=[whole() for _ in args],
        out_specs=[hbm(), whole(), whole(), whole()],
        scratch_shapes=[pltpu.SemaphoreType.DMA],
        compiler_params=pltpu.CompilerParams(vmem_limit_bytes=12 << 20),
        cost_estimate=inter_cost(width, span, 2),
        name="near_other",
    )(*args)


def far_other(head_dim, scale_b, scale_c, b, w, rows, x, dy, carry, sub, gb, gc, slab, out, parts):
    span, width = slab.shape
    every = 2
    sends = width // SLAB // every
    args = [b, w, rows, x, dy, carry, sub, gb, gc, slab]
    return pl.pallas_call(
        functools.partial(far_other_kernel, head_dim, len(parts), every, scale_b, scale_c),
        out_shape=[jax.ShapeDtypeStruct(v.shape, v.dtype) for v in (out, gb, gc)],
        in_specs=[whole() for _ in args] + [hbm()] + [whole() for _ in parts],
        out_specs=[hbm(), hbm(), hbm()],
        scratch_shapes=[
            pltpu.VMEM((span, width), BF16),
            pltpu.VMEM(gb.shape, F32),
            pltpu.VMEM(gc.shape, F32),
            pltpu.SemaphoreType.DMA((sends,)),
            pltpu.SemaphoreType.DMA((3,)),
        ],
        input_output_aliases={len(args): 0},
        compiler_params=pltpu.CompilerParams(vmem_limit_bytes=12 << 20),
        cost_estimate=inter_cost(width, span, 2),
        name="far_other",
    )(*args, out, *parts)


def local(inputs, out_grad, step_size, log_decay, b_matrix, c_matrix, skip_gain, lengths):
    x, dy = inputs[0], out_grad[0]
    tokens, columns = x.shape
    heads = step_size.shape[1]
    states = b_matrix.shape[1]
    head_dim = columns // heads
    count = lax.axis_size("seq")
    units = count // 2
    if tokens != SPAN or count % 4:
        raise ValueError("unsupported sizes")
    scale_b = 1.0 / math.sqrt(columns)
    scale_c = math.sqrt(states / (columns * count * tokens))
    def swap(v, bit):
        return lax.ppermute(v, "seq", [(i, i ^ bit) for i in range(count)])

    fixed = lambda v: pltpu.with_memory_space_constraint(v, pltpu.HBM)
    small = [fixed(v) for v in (log_decay[0], step_size[0], b_matrix[0], c_matrix[0])]
    msg, sub1_other, ld, dt, b, c, *other = first_part(lengths, *small, fixed(x), fixed(dy))
    y1 = swap(msg, 1)
    xs, subs, send, sub2_other, d, cb, *tables = own_part(
        lengths, skip_gain, ld, dt, b, c, other, x, dy
    )
    own, other = tables[:5], other + tables[5:]
    calls = 3
    pairs = heads // 4 // calls
    parts = {OTHER: [], OWN: []}

    def block(rel, k, mix, after=()):
        table = own if rel == OWN else other
        part, mix = intra(
            rel, k * pairs, pairs, head_dim, lengths, table[2], table[3], cb, table[4], x, dy, mix, after
        )
        parts[rel].append(part)
        return mix

    tile = xs.shape[1:]
    order = [(OWN, 0), (OWN, 1), (OWN, 2), (OTHER, 0), (OTHER, 1), (OTHER, 2)]
    mix = block(*order[0], None)
    if units == 4:
        (m1,) = small_call(
            functools.partial(total_kernel, False), "total", [msg.shape], d.shape, 1,
            [y1, d, xs, y1], [mix],
        )
        r1 = swap(m1, 2)
        y2 = swap(send, 1)
        mix = block(*order[1], mix, [m1])
        mix = block(*order[2], mix)
        far, own1, send1 = small_call(
            near_kernel, "near", [tile] * 3, d.shape, 2, [y1, d, xs, y1, r1], [mix]
        )
        r3 = swap(far, 4)
        mix = block(*order[3], mix, [far])
        (m2,) = small_call(
            functools.partial(total_kernel, True), "total", [tile], d.shape, 1, [y1, d, xs, y2], [mix]
        )
        r2 = swap(m2, 2)
        got1 = swap(send1, 1)
        mix = block(*order[4], mix, [m2])
        mix = block(*order[5], mix)
        own2, send2 = small_call(
            far_kernel, "far", [tile] * 2, d.shape, 2, [y1, d, xs, y2, r1, r2, r3], [mix]
        )
    else:
        y2 = swap(send, 1)
        for item in order[1:]:
            mix = block(*item, mix)
        (own1, send1), (own2, send2) = gathered(units, d, xs[0], xs[1], y1, y2)
        got1 = swap(send1, 1)
    got2 = swap(send2, 1)
    slab, gb, gc = inter_own(
        head_dim, lengths, b, c, *own[:2], x, dy, own1, own2, subs, mix, parts[OWN]
    )
    table = other[:2]
    out, slab, gb, gc = near_other(
        head_dim, b, *table, x, dy, got1, sub1_other, gb, gc, slab, parts[OTHER]
    )
    out, gb, gc = far_other(
        head_dim, scale_b, scale_c, b, *table, x, dy, got2, sub2_other, gb, gc, slab, out, parts[OTHER]
    )
    return (out[None], gb[None], gc[None])


def gathered(units, d, x1, x2, y1, y2):
    idx = lax.axis_index("seq")
    mine, unit = idx % 2, idx // 2
    lower = unit < units // 2
    tiles = x1.shape[0]
    dp = wide_rows(y1, tiles)[:, None, :]
    d = d[:, None, :]
    ys = (y1[:tiles].astype(F32), y2.astype(F32))
    xs = (x1, x2)
    totals = [pair_total(pair_flags(k == 1), d, dp, xs[k], ys[k]) for k in range(2)]
    own_half = lambda v: jnp.take(lax.all_gather(v, "seq"), 2 * jnp.arange(units) + mine, axis=0)
    forward = own_half(jnp.where(lower, totals[0], totals[1]))
    backward = own_half(jnp.where(lower, totals[1], totals[0]))
    decays = own_half(d * dp)
    state = grad = jnp.zeros_like(x1)
    for u in range(units):
        state = jnp.where(u < unit, decays[u] * state + forward[u], state)
        v = units - 1 - u
        grad = jnp.where(v > unit, decays[v] * grad + backward[v], grad)
    carries = (jnp.where(lower, state, grad), jnp.where(lower, grad, state))
    outs = [hand_on(pair_flags(k == 1), d, dp, xs[k], ys[k], carries[k]) for k in range(2)]
    return [[v.astype(BF16) for v in pair] for pair in outs]


def solution(mesh):
    placed = (
        P("batch", "seq", None),
        P("batch", "seq", None),
        P("batch", None, "seq"),
        P("batch", None, "seq"),
        P("batch", None, "seq"),
        P("batch", None, "seq"),
        P(),
        P("batch"),
    )
    return jax.shard_map(
        local,
        mesh=mesh,
        in_specs=placed,
        out_specs=(P("batch", "seq", None), P("batch", None, "seq"), P("batch", None, "seq")),
        check_vma=False,
    )
```

```python
import functools
import math

import jax
import jax.numpy as jnp
from jax import lax
from jax.experimental import pallas as pl
from jax.experimental.pallas import tpu as pltpu
from jax.sharding import PartitionSpec as P


SPAN = 256
LANES = 128
SLAB = 2 * LANES
LOG2E = math.log2(math.e)
F32 = jnp.float32
BF16 = jnp.bfloat16
NT = (((1,), (1,)), ((), ()))
TN = (((0,), (0,)), ((), ()))
OTHER, OWN = 0, 1


def place():
    idx = lax.axis_index("seq")
    count = lax.axis_size("seq")
    return idx, lax.rem(idx, 2), idx < count // 2


def mm(a, b, dims=None):
    if dims is None:
        return jnp.dot(a, b, preferred_element_type=F32)
    return lax.dot_general(a, b, dims, preferred_element_type=F32)


def pick(condition, a, b):
    if isinstance(condition, bool):
        return a if condition else b
    return jnp.where(condition, a, b)


def whole():
    return pl.BlockSpec(memory_space=pltpu.VMEM)


def smem():
    return pl.BlockSpec(memory_space=pltpu.SMEM)


def hbm():
    return pl.BlockSpec(memory_space=pltpu.HBM)


def iota(shape, axis):
    return lax.broadcasted_iota(jnp.int32, shape, axis)


def running_sum(values):
    rows, span = values.shape
    sub = span // 2
    high = values.astype(BF16)
    rest = values - high.astype(F32)
    middle = rest.astype(BF16)
    low = (rest - middle.astype(F32)).astype(BF16)
    upper = (iota((sub, sub), 0) <= iota((sub, sub), 1)).astype(F32).astype(BF16)
    pieces = jnp.concatenate([high, middle, low], axis=0)
    halves = []
    for s in range(2):
        sums = mm(pieces[:, s * sub : (s + 1) * sub], upper)
        halves.append(sums[:rows] + sums[rows : 2 * rows] + sums[2 * rows :])
    return jnp.concatenate(halves, axis=1)


def weights(ld, dt, valid):
    cum = running_sum(ld)
    _, span = cum.shape
    sub = span // 2
    end_a, end_b = cum[:, sub - 1 : sub], cum[:, span - 1 : span]
    ends = jnp.where(iota(cum.shape, 1) < sub, end_a, end_b)
    into_grad = jnp.where(iota(cum.shape, 1) < valid, jnp.exp(cum), 0.0)
    return cum, dt * jnp.exp(ends - cum), into_grad, jnp.exp(end_a), jnp.exp(end_b)


def spread(column, scratch_ref, head_dim):
    rows = scratch_ref.shape[0]
    scratch_ref[...] = jnp.broadcast_to(column, scratch_ref.shape)
    even = scratch_ref[pl.ds(0, rows // 2, stride=2), :]
    odd = scratch_ref[pl.ds(1, rows // 2, stride=2), :]
    return jnp.where(iota(even.shape, 1) < head_dim, even, odd)


def run_task(is_state, weight, read, chunks, head_dim, mat, w_ref, rows_ref, put, span, width):
    sub = span // 2
    states = mat.shape[0]
    per = SLAB // head_dim
    low = iota((states, LANES), 1) < head_dim
    w_ref[...] = weight
    chunk = width // chunks
    for g in range(width // SLAB):
        if g * SLAB % chunk == 0:
            read(None, g * SLAB // chunk)
        lhs = jnp.concatenate(
            [(mat * w_ref[pl.ds(per * g + j, 1), :]).astype(BF16) for j in range(per)], axis=0
        )
        parts = [mm(lhs[:, s * sub : (s + 1) * sub], read(s, g)) for s in range(2)]
        for q in range(2):
            lanes = slice(q * LANES, (q + 1) * LANES)
            top = slice(2 * q * states, (2 * q + 1) * states)
            bottom = slice((2 * q + 1) * states, (2 * q + 2) * states)
            e0, e1 = [jnp.where(low, p[top, lanes], p[bottom, lanes]) for p in parts]
            j = 2 * g + q
            d_a, d_b = rows_ref[0, pl.ds(j, 1), :], rows_ref[1, pl.ds(j, 1), :]
            if isinstance(is_state, bool):
                total = d_b * e0 + e1 if is_state else e0 + d_a * e1
            else:
                total = jnp.where(is_state, d_b, 1.0) * e0 + jnp.where(is_state, 1.0, d_a) * e1
            put(j, total, pick(is_state, e0, e1))


def first_kernel(
    head_dim, len_ref, ld_hbm, dt_hbm, b_hbm, c_hbm, x_ref, dy_ref,
    msg_ref, sub_ref, ld_ref, dt_ref, b_ref, c_ref, w_ref, rows_ref, row_ref,
    data_ref, task_w_ref, spread_ref, sems, small_sems
):
    idx, mine, lower = place()
    span = ld_ref.shape[1]
    sub = span // 2
    half_heads = ld_ref.shape[0] // 2
    width = data_ref.shape[1]
    chunks = sems.shape[0]
    chunk = width // chunks
    small = [
        pltpu.make_async_copy(src, dst, small_sems.at[i])
        for i, (src, dst) in enumerate(
            ((ld_hbm, ld_ref), (dt_hbm, dt_ref), (b_hbm, b_ref), (c_hbm, c_ref))
        )
    ]
    for copy in small:
        copy.start()

    def fetch(i, src):
        start = pl.multiple_of((1 - mine) * width + i * chunk, LANES)
        return pltpu.make_async_copy(
            src.at[:, pl.ds(start, chunk)], data_ref.at[:, pl.ds(i * chunk, chunk)], sems.at[i]
        )

    for i in range(chunks):

        @pl.when(lower)
        def _():
            fetch(i, x_ref).start()

        @pl.when(jnp.logical_not(lower))
        def _():
            fetch(i, dy_ref).start()

    for copy in small:
        copy.wait()
    rows = pl.ds(pl.multiple_of((1 - mine) * half_heads, 8), half_heads)
    valid = len_ref[0] - idx * span
    cum, ws, wg, d_a, d_b = weights(ld_ref[rows, :], dt_ref[rows, :], valid)
    w_ref[0] = ws
    w_ref[1] = wg
    row_ref[...] = cum * LOG2E
    rows_a = spread(d_a, spread_ref, head_dim)
    rows_b = spread(d_b, spread_ref, head_dim)
    rows_ref[0] = rows_a
    rows_ref[1] = rows_b
    tiles = sub_ref.shape[0]
    extra = narrow_rows(rows_a * rows_b)
    msg_ref[tiles:] = extra.reshape((msg_ref.shape[0] - tiles,) + msg_ref.shape[1:])

    def read(s, g):
        if s is None:
            return fetch(g, x_ref).wait()
        return data_ref[pl.ds(s * sub, sub), pl.ds(g * SLAB, SLAB)]

    def put(j, total, part):
        msg_ref[j] = total.astype(BF16)
        sub_ref[j] = part

    mat = jnp.where(lower, b_ref[...].astype(F32), c_ref[...].astype(F32))
    run_task(
        lower, jnp.where(lower, ws, wg), read, chunks, head_dim, mat, task_w_ref, rows_ref, put, span, width
    )


def first_part(length, ld, dt, b, c, x, dy):
    heads, span = ld.shape
    columns = x.shape[1]
    states = b.shape[0]
    tiles = columns // 2 // LANES
    pairs = heads // 4
    shape = jax.ShapeDtypeStruct
    tile = lambda n, t: shape((n, states, LANES), t)
    same = lambda a: shape(a.shape, a.dtype)
    outs = [
        tile(tiles + 2 * pairs // states, BF16),
        tile(tiles, F32),
        same(ld), same(dt), same(b), same(c),
    ] + table_shapes(heads, span)[:3]
    return pl.pallas_call(
        functools.partial(first_kernel, columns // heads),
        out_shape=outs,
        in_specs=[smem()] + [hbm() for _ in range(6)],
        out_specs=[whole() for _ in outs],
        scratch_shapes=[
            pltpu.VMEM((span, columns // 2), BF16),
            pltpu.VMEM((heads // 2, span), F32),
            pltpu.VMEM((heads // 2, LANES), F32),
            pltpu.SemaphoreType.DMA((4,)),
            pltpu.SemaphoreType.DMA((4,)),
        ],
        compiler_params=pltpu.CompilerParams(vmem_limit_bytes=8 << 20),
        name="first",
    )(length, ld, dt, b, c, x, dy)


def more_tables(half, head_dim, row, dt_ref, skip_ref, col_ref, skip_rows_ref):
    half_heads = row.shape[0]
    low = iota((1, LANES), 1) < head_dim
    rows = pl.ds(pl.multiple_of(half * half_heads, 8), half_heads)
    col_ref[...] = (row - jnp.log(dt_ref[rows, :]) * LOG2E).T
    for j in range(half_heads // 2):
        at = half * half_heads + 2 * j
        skip_rows_ref[pl.ds(j, 1), :] = jnp.where(low, skip_ref[at], skip_ref[at + 1])


def own_kernel(
    head_dim, len_ref, skip_ref, ld_ref, dt_ref, b_ref, c_ref, wo_ref, rowso_ref, rowo_ref, x_ref, dy_ref,
    xs_ref, subs_ref, send_ref, subo_ref, d_ref, cb_ref,
    w_ref, rows_ref, row_ref, col_ref, skip_rows_ref, colo_ref, skipo_ref,
    task_w_ref, spread_ref
):
    idx, mine, lower = place()
    span = ld_ref.shape[1]
    half_heads = ld_ref.shape[0] // 2
    width = x_ref.shape[1] // 2
    sub = span // 2
    valid = len_ref[0] - idx * span
    rows = pl.ds(pl.multiple_of(mine * half_heads, 8), half_heads)
    cum, ws, wg, d_a, d_b = weights(ld_ref[rows, :], dt_ref[rows, :], valid)
    w_ref[0] = ws
    w_ref[1] = wg
    rows_ref[0] = spread(d_a, spread_ref, head_dim)
    rows_ref[1] = spread(d_b, spread_ref, head_dim)
    row = cum * LOG2E
    row_ref[...] = row
    d_ref[...] = rows_ref[0] * rows_ref[1]
    more_tables(mine, head_dim, row, dt_ref, skip_ref, col_ref, skip_rows_ref)
    more_tables(1 - mine, head_dim, rowo_ref[...], dt_ref, skip_ref, colo_ref, skipo_ref)
    for s in range(2):
        cols = slice(s * sub, (s + 1) * sub)
        dots = mm(b_ref[:, cols], c_ref[:, cols], TN)
        t, u = iota(dots.shape, 0), iota(dots.shape, 1)
        cb_ref[s] = jnp.where(jnp.logical_and(u >= t, u + s * sub < valid), dots, 0.0)
    b, c = b_ref[...].astype(F32), c_ref[...].astype(F32)
    kind_slot = jnp.where(lower, 0, 1)

    def reader(ref, half):
        def read(s, g):
            if s is None:
                return None
            start = pl.multiple_of(half * width + g * SLAB, LANES)
            return ref[pl.ds(s * sub, sub), pl.ds(start, SLAB)]

        return read

    def putter(slot):
        def put(j, total, part):
            xs_ref[slot, j] = total
            subs_ref[slot, j] = part

        return put

    def put_other(j, total, part):
        send_ref[j] = total.astype(BF16)
        subo_ref[j] = part

    run_task(
        True, ws, reader(x_ref, mine), 1, head_dim, b, task_w_ref.at[0], rows_ref, putter(kind_slot), span, width
    )
    run_task(
        False, wg, reader(dy_ref, mine), 1, head_dim, c, task_w_ref.at[1], rows_ref,
        putter(1 - kind_slot), span, width,
    )
    upper = jnp.logical_not(lower)
    read_x, read_dy = reader(x_ref, 1 - mine), reader(dy_ref, 1 - mine)

    def read_either(s, g):
        return None if s is None else jnp.where(upper, read_x(s, g), read_dy(s, g))

    run_task(
        upper, jnp.where(upper, wo_ref[0], wo_ref[1]), read_either, 1, head_dim, jnp.where(upper, b, c),
        task_w_ref.at[2], rowso_ref, put_other, span, width,
    )


def table_shapes(heads, span):
    shape = jax.ShapeDtypeStruct
    half, pairs = heads // 2, heads // 4
    return [
        shape((2, half, span), F32),
        shape((2, pairs, LANES), F32),
        shape((half, span), F32),
        shape((span, half), F32),
        shape((pairs, LANES), F32),
    ]


def own_part(length, skip, ld, dt, b, c, other, x, dy):
    heads, span = ld.shape
    columns = x.shape[1]
    states = b.shape[0]
    pairs = heads // 4
    sub = span // 2
    tiles = columns // 2 // LANES
    shape = jax.ShapeDtypeStruct
    outs = [shape((2, tiles, states, LANES), F32)] * 2
    outs += [shape((tiles, states, LANES), BF16), shape((tiles, states, LANES), F32)]
    outs += [shape((pairs, LANES), F32), shape((2, sub, sub), F32)]
    outs += table_shapes(heads, span) + table_shapes(heads, span)[3:]
    return pl.pallas_call(
        functools.partial(own_kernel, columns // heads),
        out_shape=outs,
        in_specs=[smem(), smem()] + [whole() for _ in range(9)],
        out_specs=[whole() for _ in outs],
        scratch_shapes=[
            pltpu.VMEM((3, heads // 2, span), F32),
            pltpu.VMEM((heads // 2, LANES), F32),
        ],
        compiler_params=pltpu.CompilerParams(vmem_limit_bytes=8 << 20),
        name="own",
    )(length, skip, ld, dt, b, c, *other, x, dy)


def pair_flags(second):
    _, mine, lower = place()
    ahead = jnp.where(lower, mine == 0, mine == 1)
    return jnp.logical_not(ahead) if second else ahead


def inner_unit():
    unit = lax.axis_index("seq") // 2
    return jnp.logical_or(unit == 1, unit == 2)


def wide_rows(ref, tiles):
    both = ref[tiles:]
    both = both.reshape(both.shape[0] * both.shape[1], LANES).astype(F32)
    count = both.shape[0] // 2
    return both[:count] + both[count:]


def narrow_rows(rows):
    high = rows.astype(BF16).astype(F32)
    return jnp.concatenate([high, rows - high], axis=0).astype(BF16)


def pair_total(ahead, d, dp, x, y):
    return jnp.where(ahead, dp, d) * jnp.where(ahead, x, y) + jnp.where(ahead, y, x)


def hand_on(ahead, d, dp, x, y, carry):
    passed = jnp.where(ahead, d, dp) * carry + jnp.where(ahead, x, y)
    return jnp.where(ahead, carry, passed), jnp.where(ahead, passed, carry)


def total_kernel(second, decay_ref, mine_ref, x_ref, y_ref, *refs):
    out_ref, dp_ref = refs[-2:]
    ahead = pair_flags(second)
    tiles = x_ref.shape[1]
    dp_ref[...] = wide_rows(decay_ref, tiles)
    if not second:
        rows = narrow_rows(dp_ref[...] * mine_ref[...])
        out_ref[tiles:] = rows.reshape((out_ref.shape[0] - tiles,) + out_ref.shape[1:])
    for j in range(tiles):
        dp, d = dp_ref[pl.ds(j, 1), :], mine_ref[pl.ds(j, 1), :]
        total = pair_total(ahead, d, dp, x_ref[int(second), j], y_ref[j].astype(F32))
        out_ref[j] = total.astype(BF16)


def near_kernel(decay_ref, mine_ref, x_ref, y_ref, r_ref, *refs):
    msg_ref, own_ref, send_ref, dp_ref, pd_ref = refs[-5:]
    ahead = pair_flags(False)
    inner = inner_unit()
    tiles = x_ref.shape[1]
    dp_ref[...] = wide_rows(decay_ref, tiles)
    pd_ref[...] = wide_rows(r_ref, tiles)
    for j in range(tiles):
        dp, d, pd = dp_ref[pl.ds(j, 1), :], mine_ref[pl.ds(j, 1), :], pd_ref[pl.ds(j, 1), :]
        x, y, got = x_ref[0, j], y_ref[j].astype(F32), r_ref[j].astype(F32)
        total = pair_total(ahead, d, dp, x, y)
        joined = jnp.where(inner, d * dp, pd) * jnp.where(inner, got, total) + jnp.where(
            inner, total, got
        )
        msg_ref[j] = joined.astype(BF16)
        own, send = hand_on(ahead, d, dp, x, y, jnp.where(inner, got, 0.0))
        own_ref[j] = own.astype(BF16)
        send_ref[j] = send.astype(BF16)


def far_kernel(decay_ref, mine_ref, x_ref, y_ref, r_ref, r2_ref, far_ref, *refs):
    own_ref, send_ref, dp_ref, pd_ref = refs[-4:]
    ahead = pair_flags(True)
    inner = inner_unit()
    tiles = x_ref.shape[1]
    dp_ref[...] = wide_rows(decay_ref, tiles)
    pd_ref[...] = wide_rows(r_ref, tiles)
    for j in range(tiles):
        dp, d, pd = dp_ref[pl.ds(j, 1), :], mine_ref[pl.ds(j, 1), :], pd_ref[pl.ds(j, 1), :]
        x, y = x_ref[1, j], y_ref[j].astype(F32)
        far = far_ref[j].astype(F32)
        carry = jnp.where(inner, far, r2_ref[j].astype(F32) + pd * far)
        own, send = hand_on(ahead, d, dp, x, y, carry)
        own_ref[j] = own.astype(BF16)
        send_ref[j] = send.astype(BF16)


def small_call(kernel, outs, rows_shape, scratch, args, after=()):
    return pl.pallas_call(
        kernel,
        out_shape=[jax.ShapeDtypeStruct(o, BF16) for o in outs],
        in_specs=[whole() for _ in args] + [pl.BlockSpec(memory_space=pl.ANY) for _ in after],
        out_specs=[whole() for _ in outs],
        scratch_shapes=[pltpu.VMEM(rows_shape, F32)] * scratch,
        compiler_params=pltpu.CompilerParams(vmem_limit_bytes=4 << 20),
    )(*args, *after)


def intra_kernel(rel, pair0, pairs, head_dim, first, len_ref, row_ref, col_ref, cb_ref, skip_ref, x_ref, dy_ref, *refs):
    mix_in = None if first else refs[0]
    part_ref, mix_ref, split_ref = refs[-3:]
    sub = cb_ref.shape[1]
    idx, mine, _ = place()
    base = (mine if rel == OWN else 1 - mine) * (x_ref.shape[1] // 2)
    valid = len_ref[0] - idx * x_ref.shape[0]
    lane = iota((1, LANES), 1)
    keep = [
        (lane < head_dim).astype(F32).astype(BF16),
        (lane >= head_dim).astype(F32).astype(BF16),
    ]
    for s in range(2):
        here = pl.ds(s * sub, sub)
        acc = None if first else mix_in[s]
        inside = iota((sub, LANES), 0) + s * sub < valid
        for p in range(pairs):
            cols = pl.ds(pl.multiple_of(base + (pair0 + p) * LANES, LANES), LANES)
            xs = x_ref[here, cols]
            ys = dy_ref[here, cols]
            split_ref[p % 2, :sub, :] = ys * keep[0]
            split_ref[p % 2, sub:, :] = ys * keep[1]
            scores = mm(xs, split_ref[p % 2], NT)
            kernels = []
            for j in range(2):
                h = 2 * (pair0 + p) + j
                row = row_ref[pl.ds(h, 1), here]
                col = col_ref[here, pl.ds(h, 1)]
                decay = jnp.exp2(jnp.minimum(row - col, 100.0))
                kernels.append((decay * cb_ref[s]).astype(BF16))
                term = decay * scores[:, j * sub : (j + 1) * sub]
                acc = term if acc is None else acc + term
            within = mm(jnp.concatenate(kernels, axis=1), split_ref[p % 2])
            skip = skip_ref[pl.ds(pair0 + p, 1), :]
            part_ref[here, pl.ds(p * LANES, LANES)] = (
                within + jnp.where(inside, skip * ys.astype(F32), 0.0)
            ).astype(part_ref.dtype)
        mix_ref[s] = acc


def intra(rel, pair0, pairs, head_dim, length, row, col, cb, skip, x, dy, mix, after=()):
    span = x.shape[0]
    args = [row, col, cb, skip, x, dy] + ([] if mix is None else [mix])
    heads = 2 * pairs
    return pl.pallas_call(
        functools.partial(intra_kernel, rel, pair0, pairs, head_dim, mix is None),
        out_shape=[
            jax.ShapeDtypeStruct((span, pairs * LANES), BF16),
            jax.ShapeDtypeStruct(cb.shape, F32),
        ],
        in_specs=[smem()] + [whole() for _ in args] + [pl.BlockSpec(memory_space=pl.ANY) for _ in after],
        out_specs=[whole(), whole()],
        scratch_shapes=[pltpu.VMEM((2, span, LANES), BF16)],
        compiler_params=pltpu.CompilerParams(vmem_limit_bytes=8 << 20),
        cost_estimate=pl.CostEstimate(
            flops=heads * 2 * span * span * 128,
            transcendentals=heads * span * span // 2,
            bytes_accessed=heads * head_dim * span * 2 * 3,
        ),
        name="intra",
    )(length, *args, *after)


def pair_tiles(ref, g):
    return jnp.concatenate([ref[2 * g], ref[2 * g + 1]], axis=1)


def pair_rows(rows_ref, k, g):
    return jnp.concatenate(
        [rows_ref[k, pl.ds(2 * g, 1), :], rows_ref[k, pl.ds(2 * g + 1, 1), :]], axis=1
    )


def carry_pass(is_grad, carry_ref, sub_ref, data_ref, b_ref, w_ref, rows_ref, parts, buf_ref, base, head_dim, done):
    span, width = data_ref.shape[0], data_ref.shape[1] // 2
    sub = span // 2
    states = b_ref.shape[0]
    per = SLAB // head_dim
    rowhead = iota((per * states, SLAB), 0) // states
    lanehead = iota((per * states, SLAB), 1) // head_dim
    diag = (rowhead == lanehead).astype(F32).astype(BF16)
    b = b_ref[...].astype(F32) if is_grad else None
    slab_width = parts[0].shape[1] if is_grad else width
    total = [None, None]
    for g in range(width // SLAB):
        carry = pair_tiles(carry_ref, g)
        moved = pair_tiles(sub_ref, g) + pair_rows(rows_ref, int(is_grad), g) * carry.astype(F32)
        carries = [moved.astype(BF16), carry] if is_grad else [carry, moved.astype(BF16)]
        data_cols = pl.ds(pl.multiple_of(base + g * SLAB, LANES), SLAB)
        for s in range(2):
            here = pl.ds(s * sub, sub)
            rows = [w_ref[1 - int(is_grad), pl.ds(per * g + i, 1), here] for i in range(per)]
            spread_out = jnp.concatenate([carries[s]] * per, axis=0) * diag
            if is_grad:
                bs = b[:, s * sub : (s + 1) * sub]
                left = jnp.concatenate([(bs * r).astype(BF16) for r in rows], axis=0)
                across = mm(left, spread_out, TN)
                part = parts[g * SLAB // slab_width][here, pl.ds(g * SLAB % slab_width, SLAB)]
                buf_ref[here, pl.ds(g * SLAB, SLAB)] = (part.astype(F32) + across).astype(BF16)
            terms = mm(spread_out, data_ref[here, data_cols], NT)
            for i in range(per):
                term = rows[i] * terms[i * states : (i + 1) * states]
                total[s] = term if total[s] is None else total[s] + term
        done(g)
    return jnp.concatenate(total, axis=1)


class Sender:
    def __init__(self, buf_ref, out_ref, sems, base, every):
        self.buf_ref, self.out_ref, self.sems = buf_ref, out_ref, sems
        self.base, self.every, self.copies = base, every, []

    def __call__(self, g):
        if (g + 1) % self.every == 0:
            wide = self.every * SLAB
            k = len(self.copies)
            copy = pltpu.make_async_copy(
                self.buf_ref.at[:, pl.ds(k * wide, wide)],
                self.out_ref.at[:, pl.ds(pl.multiple_of(self.base + k * wide, LANES), wide)],
                self.sems.at[k],
            )
            copy.start()
            self.copies.append(copy)

    def wait(self):
        for copy in self.copies:
            copy.wait()


def inter_own_kernel(
    head_dim, slabs, len_ref, b_ref, c_ref, w_ref, rows_ref, x_ref, dy_ref, one_ref, two_ref,
    subs_ref, mix_ref, *refs
):
    idx, mine, lower = place()
    parts = refs[:slabs]
    buf_ref, gb_ref, gc_ref, pick_ref = refs[slabs:]
    span, width = x_ref.shape[0], x_ref.shape[1] // 2
    sub = span // 2
    base = mine * width
    valid = len_ref[0] - idx * span
    for j in range(one_ref.shape[0]):
        pick_ref[0, j] = jnp.where(lower, two_ref[j], one_ref[j])
        pick_ref[1, j] = jnp.where(lower, one_ref[j], two_ref[j])
    slot = jnp.where(lower, 0, 1)
    gb = carry_pass(
        True, pick_ref.at[0], subs_ref.at[1 - slot], x_ref, b_ref, w_ref, rows_ref, parts, buf_ref, base,
        head_dim, lambda g: None,
    )
    gc = carry_pass(
        False, pick_ref.at[1], subs_ref.at[slot], dy_ref, b_ref, w_ref, rows_ref, None, None, base,
        head_dim, lambda g: None,
    )
    mixed_b, mixed_c = [], []
    for s in range(2):
        here = slice(s * sub, (s + 1) * sub)
        t, u = iota((sub, sub), 0), iota((sub, sub), 1)
        mix = jnp.where(jnp.logical_and(u >= t, u + s * sub < valid), mix_ref[s], 0.0)
        high = mix.astype(BF16)
        rest = (mix - high.astype(F32)).astype(BF16)
        bs, cs = b_ref[:, here], c_ref[:, here]
        mixed_b.append(mm(cs, high, NT) + mm(cs, rest, NT))
        mixed_c.append(mm(bs, high) + mm(bs, rest))
    gb_ref[...] = gb + jnp.concatenate(mixed_b, axis=1)
    gc_ref[...] = gc + jnp.concatenate(mixed_c, axis=1)


def near_other_kernel(
    head_dim, slabs, b_ref, w_ref, rows_ref, x_ref, dy_ref, carry_ref, sub_ref, gb_in, gc_in, slab_ref, *refs
):
    _, mine, lower = place()
    parts = refs[:slabs]
    out_ref, buf_ref, gb_ref, gc_ref, sem = refs[slabs:]
    width = x_ref.shape[1] // 2
    base = (1 - mine) * width
    start = pl.multiple_of(mine * width, LANES)
    own_copy = pltpu.make_async_copy(slab_ref, out_ref.at[:, pl.ds(start, width)], sem)
    own_copy.start()
    gb_ref[...] = gb_in[...]
    gc_ref[...] = gc_in[...]

    @pl.when(jnp.logical_not(lower))
    def _():
        gb_ref[...] += carry_pass(
            True, carry_ref, sub_ref, x_ref, b_ref, w_ref, rows_ref, parts, buf_ref, base, head_dim,
            lambda g: None,
        )

    @pl.when(lower)
    def _():
        gc_ref[...] += carry_pass(
            False, carry_ref, sub_ref, dy_ref, b_ref, w_ref, rows_ref, None, None, base, head_dim,
            lambda g: None,
        )

    own_copy.wait()


def far_other_kernel(
    head_dim, slabs, every, scale_b, scale_c, b_ref, w_ref, rows_ref, x_ref, dy_ref, carry_ref, sub_ref,
    gb_in, gc_in, slab_ref, out_in, *refs
):
    _, mine, lower = place()
    parts = refs[:slabs]
    out_ref, gb_out, gc_out, buf_ref, gb_ref, gc_ref, sems, small_sems = refs[slabs:]
    width = x_ref.shape[1] // 2
    base = (1 - mine) * width
    gb_ref[...] = gb_in[...] * scale_b
    gc_ref[...] = gc_in[...] * scale_c
    copies = [
        pltpu.make_async_copy(src, dst, small_sems.at[i])
        for i, (src, dst) in enumerate(((gb_ref, gb_out), (gc_ref, gc_out)))
    ]

    @pl.when(lower)
    def _():
        send = Sender(buf_ref, out_ref, sems, base, every)
        gb_ref[...] += scale_b * carry_pass(
            True, carry_ref, sub_ref, x_ref, b_ref, w_ref, rows_ref, parts, buf_ref, base, head_dim, send
        )
        for copy in copies:
            copy.start()
        send.wait()

    @pl.when(jnp.logical_not(lower))
    def _():
        start = pl.multiple_of(base, LANES)
        slab_copy = pltpu.make_async_copy(slab_ref, out_ref.at[:, pl.ds(start, width)], small_sems.at[2])
        slab_copy.start()
        gc_ref[...] += scale_c * carry_pass(
            False, carry_ref, sub_ref, dy_ref, b_ref, w_ref, rows_ref, None, None, base, head_dim,
            lambda g: None,
        )
        for copy in copies:
            copy.start()
        slab_copy.wait()

    for copy in copies:
        copy.wait()


def inter_cost(width, span, passes):
    return pl.CostEstimate(
        flops=width * 2 * span * 256 * passes, transcendentals=0, bytes_accessed=width * span * 2 * 4
    )


def inter_own(head_dim, length, b, c, w, rows, x, dy, one, two, subs, mix, parts):
    states = b.shape[0]
    span, width = x.shape[0], x.shape[1] // 2
    small = jax.ShapeDtypeStruct((states, span), F32)
    args = [b, c, w, rows, x, dy, one, two, subs, mix, *parts]
    return pl.pallas_call(
        functools.partial(inter_own_kernel, head_dim, len(parts)),
        out_shape=[jax.ShapeDtypeStruct((span, width), BF16), small, small],
        in_specs=[smem()] + [whole() for _ in args],
        out_specs=[whole(), whole(), whole()],
        scratch_shapes=[pltpu.VMEM((2,) + one.shape, BF16)],
        compiler_params=pltpu.CompilerParams(vmem_limit_bytes=12 << 20),
        cost_estimate=inter_cost(width, span, 3),
        name="inter_own",
    )(length, *args)


def near_other(head_dim, b, w, rows, x, dy, carry, sub, gb, gc, slab, parts):
    span, width = slab.shape
    args = [b, w, rows, x, dy, carry, sub, gb, gc, slab, *parts]
    return pl.pallas_call(
        functools.partial(near_other_kernel, head_dim, len(parts)),
        out_shape=[
            jax.ShapeDtypeStruct(v, t)
            for v, t in (((span, 2 * width), BF16), (slab.shape, BF16), (gb.shape, F32), (gc.shape, F32))
        ],
        in_specs=[whole() for _ in args],
        out_specs=[hbm(), whole(), whole(), whole()],
        scratch_shapes=[pltpu.SemaphoreType.DMA],
        compiler_params=pltpu.CompilerParams(vmem_limit_bytes=12 << 20),
        cost_estimate=inter_cost(width, span, 2),
        name="near_other",
    )(*args)


def far_other(head_dim, scale_b, scale_c, b, w, rows, x, dy, carry, sub, gb, gc, slab, out, parts):
    span, width = slab.shape
    every = 1
    sends = width // SLAB // every
    args = [b, w, rows, x, dy, carry, sub, gb, gc, slab]
    return pl.pallas_call(
        functools.partial(far_other_kernel, head_dim, len(parts), every, scale_b, scale_c),
        out_shape=[jax.ShapeDtypeStruct(v.shape, v.dtype) for v in (out, gb, gc)],
        in_specs=[whole() for _ in args] + [hbm()] + [whole() for _ in parts],
        out_specs=[hbm(), hbm(), hbm()],
        scratch_shapes=[
            pltpu.VMEM((span, width), BF16),
            pltpu.VMEM(gb.shape, F32),
            pltpu.VMEM(gc.shape, F32),
            pltpu.SemaphoreType.DMA((sends,)),
            pltpu.SemaphoreType.DMA((3,)),
        ],
        input_output_aliases={len(args): 0},
        compiler_params=pltpu.CompilerParams(vmem_limit_bytes=12 << 20),
        cost_estimate=inter_cost(width, span, 2),
        name="far_other",
    )(*args, out, *parts)


def device_work(inputs, out_grad, step_size, log_decay, b_matrix, c_matrix, skip_gain, lengths):
    x, dy = inputs[0], out_grad[0]
    tokens, columns = x.shape
    heads = step_size.shape[1]
    states = b_matrix.shape[1]
    head_dim = columns // heads
    count = lax.axis_size("seq")
    units = count // 2
    if tokens != SPAN or count % 4:
        raise ValueError("unsupported sizes")
    scale_b = 1.0 / math.sqrt(columns)
    scale_c = math.sqrt(states / (columns * count * tokens))

    def swap(v, bit):
        return lax.ppermute(v, "seq", [(i, i ^ bit) for i in range(count)])

    fixed = lambda v: pltpu.with_memory_space_constraint(v, pltpu.HBM)
    small = [fixed(v) for v in (log_decay[0], step_size[0], b_matrix[0], c_matrix[0])]
    msg, sub1_other, ld, dt, b, c, *other = first_part(lengths, *small, fixed(x), fixed(dy))
    y1 = swap(msg, 1)
    xs, subs, send, sub2_other, d, cb, *tables = own_part(
        lengths, skip_gain, ld, dt, b, c, other, x, dy
    )
    own, other = tables[:5], other + tables[5:]
    calls = 6
    pairs = heads // 4 // calls
    parts = {OTHER: [], OWN: []}

    def block(rel, k, mix, after=()):
        table = own if rel == OWN else other
        part, mix = intra(
            rel, k * pairs, pairs, head_dim, lengths, table[2], table[3], cb, table[4], x, dy, mix, after
        )
        parts[rel].append(part)
        return mix

    tile = xs.shape[1:]
    order = [(rel, k) for rel in (OWN, OTHER) for k in range(calls)]

    def run(count, mix, after=()):
        for _ in range(count):
            mix = block(*order.pop(0), mix, after)
            after = ()
        return mix

    mix = run(3, None)
    if units == 4:
        (m1,) = small_call(
            functools.partial(total_kernel, False), [msg.shape], d.shape, 1,
            [y1, d, xs, y1], [mix],
        )
        r1 = swap(m1, 2)
        y2 = swap(send, 1)
        mix = run(4, mix, [m1])
        far, own1, send1 = small_call(near_kernel, [tile] * 3, d.shape, 2, [y1, d, xs, y1, r1], [mix])
        r3 = swap(far, 4)
        (m2,) = small_call(functools.partial(total_kernel, True), [tile], d.shape, 1, [y1, d, xs, y2], [far])
        r2 = swap(m2, 2)
        got1 = swap(send1, 1)
        mix = run(5, mix, [m2])
        own2, send2 = small_call(far_kernel, [tile] * 2, d.shape, 2, [y1, d, xs, y2, r1, r2, r3], [mix])
    else:
        y2 = swap(send, 1)
        mix = run(len(order), mix)
        (own1, send1), (own2, send2) = gathered(units, d, xs[0], xs[1], y1, y2)
        got1 = swap(send1, 1)
    got2 = swap(send2, 1)
    slab, gb, gc = inter_own(
        head_dim, lengths, b, c, *own[:2], x, dy, own1, own2, subs, mix, parts[OWN]
    )
    table = other[:2]
    out, slab, gb, gc = near_other(
        head_dim, b, *table, x, dy, got1, sub1_other, gb, gc, slab, parts[OTHER]
    )
    out, gb, gc = far_other(
        head_dim, scale_b, scale_c, b, *table, x, dy, got2, sub2_other, gb, gc, slab, out, parts[OTHER]
    )
    return (out[None], gb[None], gc[None])


def gathered(units, d, x1, x2, y1, y2):
    idx = lax.axis_index("seq")
    mine, unit = idx % 2, idx // 2
    lower = unit < units // 2
    tiles = x1.shape[0]
    dp = wide_rows(y1, tiles)[:, None, :]
    d = d[:, None, :]
    ys = (y1[:tiles].astype(F32), y2.astype(F32))
    xs = (x1, x2)
    totals = [pair_total(pair_flags(k == 1), d, dp, xs[k], ys[k]) for k in range(2)]
    own_half = lambda v: jnp.take(lax.all_gather(v, "seq"), 2 * jnp.arange(units) + mine, axis=0)
    forward = own_half(jnp.where(lower, totals[0], totals[1]))
    backward = own_half(jnp.where(lower, totals[1], totals[0]))
    decays = own_half(d * dp)
    state = grad = jnp.zeros_like(x1)
    for u in range(units):
        state = jnp.where(u < unit, decays[u] * state + forward[u], state)
        v = units - 1 - u
        grad = jnp.where(v > unit, decays[v] * grad + backward[v], grad)
    carries = (jnp.where(lower, state, grad), jnp.where(lower, grad, state))
    outs = [hand_on(pair_flags(k == 1), d, dp, xs[k], ys[k], carries[k]) for k in range(2)]
    return [[v.astype(BF16) for v in pair] for pair in outs]


def solution(mesh):
    placed = (
        P("batch", "seq", None),
        P("batch", "seq", None),
        P("batch", None, "seq"),
        P("batch", None, "seq"),
        P("batch", None, "seq"),
        P("batch", None, "seq"),
        P(),
        P("batch"),
    )
    return jax.shard_map(
        device_work,
        mesh=mesh,
        in_specs=placed,
        out_specs=(P("batch", "seq", None), P("batch", None, "seq"), P("batch", None, "seq")),
        check_vma=False,
    )
```
